32 devices in a mesh: gx: 4 (over y, x), gy: 8 (over z, core).
Axes of the slice: x: 2, y: 2, z: 4, core: 2. Of those that a mesh axis runs over, the one named last changes fastest.
Arguments:
- volume: float32 [128, 512, 256], P('gx', 'gy'), may hold values from -18 to 18, as said below
Outputs:
- denoised: float32 [128, 512, 256], P('gx', 'gy')
The draws below stay inside these ranges and needn't reach their ends.
Inputs may be any that keep to these rules, and one draw needn't show every extreme that they name: `volume`: real values.
All inputs are finite; a program needn't handle non-finite values.
Results may differ from the reference program's by a relative error of at most 0.00002.
Values sent between devices are 32-bit elements; how exact they have to be, the bound alone decides.
A program may use at most 128 MiB of HBM per device.

```python
import math
import jax
import jax.numpy as jnp

NZ = 256
LEVELS = 3
NX = 128
NY = 512


def draw_volume(key, part):
    ramp_x = 1.0 + 2.0 * jnp.arange(NX, dtype=jnp.float32)[:, None, None] / NX
    noise = jnp.clip(jax.random.normal(key, (NX, NY, NZ), jnp.float32), -6.0, 6.0)
    return (ramp_x * noise).astype(jnp.float32)


def setup_inputs(seed: int = 0) -> dict:
    seeds = jax.random.split(jax.random.key(seed), 2)
    return {
        "volume": draw_volume(jax.random.fold_in(seeds[1], 71), 0),
    }


root_three = math.sqrt(3.0)
lift_near = math.sqrt(3.0) / 4.0
lift_far = (math.sqrt(3.0) - 2.0) / 4.0
scale_low = (math.sqrt(3.0) - 1.0) / math.sqrt(2.0)
scale_high = (math.sqrt(3.0) + 1.0) / math.sqrt(2.0)

def take_every(values, start, along):
    index = [slice(None)] * values.ndim
    index[along] = slice(start, None, 2)
    return values[tuple(index)]

def weave(first, second, along):
    stacked = jnp.stack([first, second], axis=along + 1)
    shape = list(first.shape)
    shape[along] = shape[along] * 2
    return stacked.reshape(shape)

def forward_lines(values, along):
    even_cells = take_every(values, 0, along)
    odd_cells = take_every(values, 1, along)
    smooth = even_cells + root_three * odd_cells
    detail = odd_cells - lift_near * smooth - lift_far * jnp.roll(smooth, 1, axis=along)
    smooth = smooth - jnp.roll(detail, -1, axis=along)
    return (scale_high * detail, scale_low * smooth)

def inverse_lines(detail, smooth, along):
    detail = detail / scale_high
    smooth = smooth / scale_low
    first = smooth + jnp.roll(detail, -1, axis=along)
    odd_cells = detail + lift_near * first + lift_far * jnp.roll(first, 1, axis=along)
    even_cells = first - root_three * odd_cells
    return weave(even_cells, odd_cells, along)

def forward_level(coarse):
    detail, smooth = forward_lines(coarse, 0)
    coeffs = weave(detail, smooth, 0)
    detail, smooth = forward_lines(coeffs, 1)
    coeffs = weave(detail, smooth, 1)
    detail, smooth = forward_lines(coeffs, 2)
    return jnp.concatenate([smooth, detail], axis=2)

def inverse_level(coeffs):
    half = coeffs.shape[2] // 2
    rebuilt = inverse_lines(coeffs[:, :, half:], coeffs[:, :, :half], 2)
    rebuilt = inverse_lines(take_every(rebuilt, 0, 1), take_every(rebuilt, 1, 1), 1)
    return inverse_lines(take_every(rebuilt, 0, 0), take_every(rebuilt, 1, 0), 0)

def split_view(coeffs):
    sizes = coeffs.shape
    return coeffs.reshape(sizes[0] // 2, 2, sizes[1] // 2, 2, sizes[2])

def shrink_insert(coeffs, coarse, limit):
    shrunk = coeffs - jnp.clip(coeffs, -limit, limit)
    half = coeffs.shape[2] // 2
    view = split_view(shrunk).at[:, 1, :, 1, :half].set(coarse)
    return view.reshape(coeffs.shape)

def reference(volume):
    levels = []
    coarse = volume
    for level in range(LEVELS):
        coeffs = forward_level(coarse)
        levels.append(coeffs)
        half = coeffs.shape[2] // 2
        coarse = split_view(coeffs)[:, 1, :, 1, :half]
    finest = levels[0]
    half = finest.shape[2] // 2
    diagonal = split_view(finest)[:, 0, :, 0, half:]
    count = NX * NY * NZ // 8
    noise = jnp.sum(jnp.abs(diagonal)) * (math.sqrt(math.pi / 2.0) / count)
    rebuilt = coarse
    for level in range(LEVELS - 1, -1, -1):
        coeffs = shrink_insert(levels[level], rebuilt, noise)
        rebuilt = inverse_level(coeffs)
    return rebuilt
```

```python
import functools
import math

import jax
import jax.numpy as jnp
import numpy as np
from jax import lax
from jax.experimental import pallas as pl
from jax.experimental.pallas import tpu as pltpu
from jax.sharding import PartitionSpec as P

ROOT3 = math.sqrt(3.0)
NEAR = math.sqrt(3.0) / 4.0
FAR = (math.sqrt(3.0) - 2.0) / 4.0
LOW = (math.sqrt(3.0) - 1.0) / math.sqrt(2.0)
HIGH = (math.sqrt(3.0) + 1.0) / math.sqrt(2.0)
LANES = 128
PAD = 8


def forward_matrix(size):
    lines = np.eye(size)
    even, odd = lines[:, 0::2], lines[:, 1::2]
    smooth = even + ROOT3 * odd
    detail = odd - NEAR * smooth - FAR * np.roll(smooth, 1, 1)
    smooth = smooth - np.roll(detail, -1, 1)
    return np.concatenate([LOW * smooth, HIGH * detail], 1)


def inverse_matrix(size):
    lines = np.eye(size)
    smooth, detail = lines[:, : size // 2] / LOW, lines[:, size // 2 :] / HIGH
    first = smooth + np.roll(detail, -1, 1)
    odd = detail + NEAR * first + FAR * np.roll(first, 1, 1)
    even = first - ROOT3 * odd
    return np.stack([even, odd], 2).reshape(size, size)


def halves(matrix, size):
    full = np.zeros((size, size))
    full[: matrix.shape[0], : matrix.shape[1]] = matrix
    high = full.astype(jnp.bfloat16)
    low = (full - high.astype(np.float64)).astype(jnp.bfloat16)
    return np.stack([high, low])


def times(values, w_ref):
    high = values.astype(jnp.bfloat16)
    low = (values - high.astype(jnp.float32)).astype(jnp.bfloat16)
    dot = functools.partial(jnp.dot, preferred_element_type=jnp.float32)
    return dot(high, w_ref[0]) + (dot(low, w_ref[0]) + dot(high, w_ref[1]))


def shrink(values, noise):
    return values - jnp.clip(values, -noise, noise)


def sums(even, odd):
    smooth = even + ROOT3 * odd
    return smooth, odd - NEAR * smooth


def undo(detail, first, before):
    odd = detail + NEAR * first + FAR * before
    return first - ROOT3 * odd, odd


def weave(even, odd):
    both = jnp.stack([even, odd], axis=1)
    return both.reshape((2 * even.shape[0],) + even.shape[1:])


def forward_x(src, halo, det, smo, count):
    smooth, part = sums(src[0], src[1])
    det[0] = HIGH * (part - FAR * halo[0])

    def step(n, carry):
        before, _ = sums(src[2 * n - 2], src[2 * n - 1])
        smooth, part = sums(src[2 * n], src[2 * n + 1])
        detail = part - FAR * before
        det[n] = HIGH * detail
        smo[n - 1] = LOW * (before - detail)
        return carry

    lax.fori_loop(1, count, step, 0)
    last, _ = sums(src[2 * count - 2], src[2 * count - 1])
    smo[count - 1] = LOW * (last - (halo[1] - FAR * last))


def forward_y(load, count):
    s0, t0 = sums(load(PAD), load(PAD + 1))
    sm, _ = sums(load(PAD - 2), load(PAD - 1))
    sp, tp = sums(load(PAD + 2), load(PAD + 3))
    return HIGH * (t0 - FAR * sm), LOW * (s0 - (tp - FAR * s0))


def kernel(shape, count_all, nx, ny, vol, w1, w2, w3, v1, v2, v3, out,
           e1, hx1, sx1, xd1, xs1, s1s, s1d, d1s, d1d,
           e2, hx2, sx2, xd2, xs2, ss, sd, ds, dd, t3d, t3s, r2, r1,
           p1s, p1d, o1, ob, part, total, line, send, recv, lsem, osem):
    cx, cy, cz = shape
    ix, iy = lax.axis_index("gx"), lax.axis_index("gy")

    def device(dx, dy):
        return (lax.rem(ix + dx + nx, nx), lax.rem(iy + dy + ny, ny))

    loads = [
        pltpu.make_async_copy(
            vol.at[:, :, pl.ds(h * LANES, LANES)],
            e1.at[:, h, pl.ds(PAD, cy), :], lsem.at[h])
        for h in range(2)
    ]
    for c in loads:
        c.start()

    greet = [(dx, dy) for dx in (-1, 0, 1) for dy in (-1, 0, 1) if dx or dy]
    greet += [(dx, 0) for dx in range(2, nx - 1)] + [(0, dy) for dy in range(2, ny - 1)]
    barrier = pltpu.get_barrier_semaphore()
    for d in greet:
        pl.semaphore_signal(barrier, inc=1, device_id=device(*d),
                            device_id_type=pl.DeviceIdType.MESH)
    pl.semaphore_wait(barrier, len(greet))

    slot = [0]
    started = []

    def post(src, dst, dx, dy):
        n = slot[0]
        slot[0] += 1
        c = pltpu.make_async_remote_copy(
            src_ref=src, dst_ref=dst, send_sem=send.at[n], recv_sem=recv.at[n],
            device_id=device(dx, dy), device_id_type=pl.DeviceIdType.MESH)
        c.start()
        started.append(c)
        return c

    for c in loads:
        c.wait()

    low, high = pl.ds(0, PAD), pl.ds(PAD + cy, PAD)
    first, last = pl.ds(PAD, PAD), pl.ds(cy, PAD)
    sx1[0] = sums(e1[cx - 2, :, PAD : PAD + cy], e1[cx - 1, :, PAD : PAD + cy])[0]
    sx1[1] = sums(e1[0, :, PAD : PAD + cy], e1[1, :, PAD : PAD + cy])[1]
    round1 = []
    for side, dx in ((0, 1), (1, -1)):
        round1 += [
            post(sx1.at[side], hx1.at[side, :, pl.ds(PAD, cy), :], dx, 0),
            post(sx1.at[side, :, pl.ds(cy - PAD, PAD), :], hx1.at[side, :, low, :], dx, 1),
            post(sx1.at[side, :, pl.ds(0, PAD), :], hx1.at[side, :, high, :], dx, -1),
        ]
    round1 += [
        post(e1.at[:, :, last, :], e1.at[:, :, low, :], 0, 1),
        post(e1.at[:, :, first, :], e1.at[:, :, high, :], 0, -1),
    ]
    for c in round1:
        c.wait_recv()
    hx, hy = cx // 2, cy // 2
    forward_x(e1, hx1, xd1, xs1, hx)

    def cols1(n, carry):
        for h in range(2):
            for src, det, smo, at in ((xd1, d1d, d1s, n), (xs1, s1d, s1s, n + 1)):
                d, s = forward_y(
                    lambda start: src[n, h, pl.ds(start, hy, stride=2), :], hy)
                det[at, h, 0:hy] = d
                smo[at, h, PAD : PAD + hy] = s
        return carry

    lax.fori_loop(0, hx, cols1, 0)

    chunk = hx // 2

    def depth1(ref, x0, y0, extra=None):
        rows = jnp.concatenate(
            [ref[pl.ds(x0, chunk), h, y0 : y0 + hy].reshape(chunk * hy, LANES) for h in range(2)],
            axis=1)
        got = times(rows, w1)
        parts = [got[:, h * LANES : (h + 1) * LANES].reshape(chunk, hy, LANES) for h in range(2)]
        for h in range(2):
            ref[pl.ds(x0, chunk), h, y0 : y0 + hy] = parts[h]
        return parts

    magnitude = jnp.zeros((PAD, LANES), jnp.float32)
    for i in range(2):
        parts = depth1(s1s, 1 + i * chunk, PAD)
        e2[i * chunk : (i + 1) * chunk, PAD : PAD + hy] = parts[0]

    low2, high2 = pl.ds(0, PAD), pl.ds(PAD + hy, PAD)
    sx2[0] = sums(e2[hx - 2, PAD : PAD + hy], e2[hx - 1, PAD : PAD + hy])[0]
    sx2[1] = sums(e2[0, PAD : PAD + hy], e2[1, PAD : PAD + hy])[1]
    round2 = []
    for side, dx in ((0, 1), (1, -1)):
        round2 += [
            post(sx2.at[side], hx2.at[side, pl.ds(PAD, hy), :], dx, 0),
            post(sx2.at[side, pl.ds(hy - PAD, PAD), :], hx2.at[side, low2, :], dx, 1),
            post(sx2.at[side, pl.ds(0, PAD), :], hx2.at[side, high2, :], dx, -1),
        ]
    round2 += [
        post(e2.at[:, pl.ds(hy, PAD), :], e2.at[:, low2, :], 0, 1),
        post(e2.at[:, pl.ds(PAD, PAD), :], e2.at[:, high2, :], 0, -1),
    ]

    for i in range(2):
        depth1(s1d, 1 + i * chunk, 0)
        depth1(d1s, i * chunk, PAD)
        parts = depth1(d1d, i * chunk, 0)
        magnitude = magnitude + jnp.sum(
            jnp.abs(parts[1]).reshape(chunk * hy // PAD, PAD, LANES), axis=0)

    part[0] = magnitude
    sums_x = [post(part.at[0], part.at[k], k, 0) for k in range(1, nx)]

    for c in round2:
        c.wait_recv()
    qx, qy = hx // 2, hy // 2
    forward_x(e2, hx2, xd2, xs2, qx)

    def cols2(n, carry):
        for src, det, smo, at_d, at_s in (
            (xd2, dd, ds, n + 1, n + 1), (xs2, sd, ss, n + 2, n + 4)):
            d, s = forward_y(lambda start: src[n, pl.ds(start, qy, stride=2), :], qy)
            det[at_d, PAD : PAD + qy] = d
            smo[at_s, PAD : PAD + qy] = s
        return carry

    lax.fori_loop(0, qx, cols2, 0)

    def depth2(ref, x0):
        rows = ref[x0 : x0 + qx, PAD : PAD + qy].reshape(qx * qy, LANES)
        ref[x0 : x0 + qx, PAD : PAD + qy] = times(rows, w2).reshape(qx, qy, LANES)

    depth2(ss, 4)
    depth2(sd, 2)
    depth2(ds, 1)
    depth2(dd, 1)

    def spread(ref, own, lows, highs, up, down):
        posts = []
        rows = {0: (pl.ds(PAD, qy), pl.ds(PAD, qy))}
        if up:
            rows[1] = (pl.ds(qy, PAD), pl.ds(0, PAD))
        if down:
            rows[-1] = (pl.ds(PAD, PAD), pl.ds(PAD + qy, PAD))
        layers = {0: (pl.ds(own, qx), pl.ds(own, qx))}
        if lows:
            layers[1] = (pl.ds(own + qx - lows, lows), pl.ds(own - lows, lows))
        if highs:
            layers[-1] = (pl.ds(own, highs), pl.ds(own + qx, highs))
        for dx, (xsrc, xdst) in layers.items():
            for dy, (ysrc, ydst) in rows.items():
                if dx or dy:
                    posts.append(post(ref.at[xsrc, ysrc, :], ref.at[xdst, ydst, :], dx, dy))
        return posts

    round3 = spread(ss, 4, 4, 2, True, True)
    for c in sums_x:
        c.wait_recv()
    acc = part[0]
    for k in range(1, nx):
        acc = acc + part[k]
    total[0] = acc
    sums_y = [post(total.at[0], total.at[k], 0, k) for k in range(1, ny)]
    round4 = spread(sd, 2, 2, 0, True, True)
    round4 += spread(ds, 1, 1, 1, True, False)
    round4 += spread(dd, 1, 1, 1, True, True)

    ends = []
    for ref, own, dx in ((s1s, 1, 1), (s1d, 1, 1), (d1s, 0, -1), (d1d, 0, -1)):
        smooth = ref is s1s or ref is d1s
        x_all = pl.ds(own, hx)
        y_all = pl.ds(PAD if smooth else 0, hy)
        x_src, x_dst = (hx, 0) if dx == 1 else (0, hx)
        y_src, y_dst = (pl.ds(hy, PAD), pl.ds(0, PAD)) if smooth else (pl.ds(0, PAD), pl.ds(hy, PAD))
        dy = 1 if smooth else -1
        lanes = pl.ds(1, 1) if ref is s1s else pl.ds(0, 2)
        ends += [
            post(ref.at[pl.ds(x_src, 1), lanes, y_all, :], ref.at[pl.ds(x_dst, 1), lanes, y_all, :], dx, 0),
            post(ref.at[x_all, lanes, y_src, :], ref.at[x_all, lanes, y_dst, :], 0, dy),
            post(ref.at[pl.ds(x_src, 1), lanes, y_src, :], ref.at[pl.ds(x_dst, 1), lanes, y_dst, :], dx, dy),
        ]

    for c in round3:
        c.wait_recv()
    low_s, low_t = [], []
    for n in range(qx // 2 + 3):
        s, t = sums(ss[2 * n], ss[2 * n + 1])
        low_s.append(s)
        low_t.append(t)
    n3 = qx // 2 + 2
    for n in range(n3):
        detail = low_t[n + 1] - FAR * low_s[n]
        t3d[n] = HIGH * detail
        t3s[n] = LOW * (low_s[n] - detail)
    h3 = qy // 2 + PAD
    bands = []
    for src in (t3d, t3s):
        s, t = sums(src[:, pl.ds(0, h3, stride=2), :], src[:, pl.ds(1, h3, stride=2), :])
        d = t - FAR * pltpu.roll(s, 1, 1)
        s = s - pltpu.roll(d, h3 - 1, 1)
        bands += [HIGH * d, LOW * s]
    for i, band in enumerate(bands):
        bands[i] = times(band.reshape(n3 * h3, LANES), w3).reshape(n3, h3, LANES)

    for c in sums_y:
        c.wait_recv()
    acc = total[0]
    for k in range(1, ny):
        acc = acc + total[k]
    noise = jnp.sum(acc, axis=(0, 1), keepdims=True) * (math.sqrt(math.pi / 2.0) / count_all)
    line[...] = jnp.broadcast_to(noise, (PAD, LANES))

    lane3 = lax.broadcasted_iota(jnp.int32, (n3, h3, LANES), 2)
    noise3 = noise.reshape(1, 1, 1)
    b_dd, b_ds, b_sd = (shrink(b, noise3) for b in bands[:3])
    b_ss = jnp.where(lane3 < cz // 8, bands[3], shrink(bands[3], noise3))

    def inverse_x(det, smo):
        det, smo = det * (1.0 / HIGH), smo * (1.0 / LOW)
        one = smo + det
        even, odd = undo(det[:-1], one[1:], one[:-1])
        return weave(even, odd)

    y_d = inverse_x(b_dd, b_sd) * (1.0 / HIGH)
    y_s = inverse_x(b_ds, b_ss) * (1.0 / LOW)
    one = y_s + pltpu.roll(y_d, h3 - 1, 1)
    even, odd = undo(y_d, one, pltpu.roll(one, 1, 1))
    r2[:, pl.ds(0, h3, stride=2), :] = even
    r2[:, pl.ds(1, h3, stride=2), :] = odd
    x2, yrows = qx + 2, qy + 2 * PAD
    back = times(r2[...].reshape(x2 * yrows, LANES), v3).reshape(x2, yrows, LANES)

    for c in round4:
        c.wait_recv()
    for c in round3:
        c.wait_send()
    lane2 = lax.broadcasted_iota(jnp.int32, (x2, yrows, LANES), 2)
    ss[2 : 2 + x2] = jnp.where(lane2 < cz // 4, back, shrink(ss[2 : 2 + x2], noise3))
    noise2 = noise

    def inv2(n, carry):
        def one_x(n):
            d_d = shrink(dd[n], noise2) * (1.0 / HIGH)
            d_s = shrink(ds[n], noise2) * (1.0 / HIGH)
            s_d = shrink(sd[n], noise2) * (1.0 / LOW)
            s_s = ss[n + 2] * (1.0 / LOW)
            return d_d, d_s, s_d + d_d, s_s + d_s

        d_d, d_s, b_d, b_s = one_x(n)
        _, _, f_d, f_s = one_x(n + 1)
        pair_d = undo(d_d, f_d, b_d)
        pair_s = undo(d_s, f_s, b_s)
        for i in range(2):
            y_d, y_s = pair_d[i] * (1.0 / HIGH), pair_s[i] * (1.0 / LOW)
            one = y_s + pltpu.roll(y_d, yrows - 1, 0)
            even, odd = undo(y_d, one, pltpu.roll(one, 1, 0))
            r1[2 * n + i, pl.ds(0, yrows, stride=2), :] = even
            r1[2 * n + i, pl.ds(1, yrows, stride=2), :] = odd
        return carry

    lax.fori_loop(0, qx + 1, inv2, 0)
    x1, y1 = hx + 2, hy + PAD
    back = times(r1[:, PAD : PAD + y1].reshape(x1 * y1, LANES), v2).reshape(x1, y1, LANES)
    s1s[:, 0] = back[1:]

    for c in ends:
        c.wait_recv()

    def inv1(n, carry):
        for h in range(2):
            for det, smo, dst in ((d1d, s1d, p1d), (d1s, s1s, p1s)):
                plain = smo is s1s and h == 0

                def one_x(n):
                    d = shrink(det[n, h], noise2) * (1.0 / HIGH)
                    s = smo[n, h] if plain else shrink(smo[n, h], noise2)
                    return d, s * (1.0 / LOW) + d

                d, before = one_x(n)
                _, one = one_x(n + 1)
                even, odd = undo(d, one, before)
                dst[2 * n, h] = even
                dst[2 * n + 1, h] = odd
        return carry

    lax.fori_loop(0, hx, inv1, 0)

    def inv1_y(n, carry):
        for h in range(2):
            y_d = p1d[n, h, 0:hy] * (1.0 / HIGH)
            y_n = p1d[n, h, 1 : hy + 1] * (1.0 / HIGH)
            s = p1s[n, h, PAD : PAD + hy] * (1.0 / LOW)
            s_b = p1s[n, h, PAD - 1 : PAD - 1 + hy] * (1.0 / LOW)
            even, odd = undo(y_d, s + y_n, s_b + y_d)
            o1[n, h, pl.ds(0, hy, stride=2), :] = even
            o1[n, h, pl.ds(1, hy, stride=2), :] = odd
        return carry

    lax.fori_loop(0, cx, inv1_y, 0)
    layers = 8
    outs = []
    for i in range(cx // layers):
        xs = slice(i * layers, (i + 1) * layers)
        rows = jnp.concatenate(
            [o1[xs, h].reshape(layers * cy, LANES) for h in range(2)], axis=1)
        ob[xs] = times(rows, v1).reshape(layers, cy, cz)
        c = pltpu.make_async_copy(ob.at[xs], out.at[xs], osem.at[i])
        c.start()
        outs.append(c)
    for c in outs:
        c.wait()
    early = [id(c) for c in round3]
    for c in started:
        if id(c) not in early:
            c.wait_send()


def on_device(nx, ny, volume):
    cx, cy, cz = volume.shape
    hx, hy, qx, qy = cx // 2, cy // 2, cx // 4, cy // 4
    n3, h3 = qx // 2 + 2, qy // 2 + PAD
    f32 = jnp.float32
    count = cx * nx * cy * ny * cz // 8
    weights = [
        halves(forward_matrix(cz), cz), halves(forward_matrix(cz // 2), LANES),
        halves(forward_matrix(cz // 4), LANES), halves(inverse_matrix(cz), cz),
        halves(inverse_matrix(cz // 2), LANES), halves(inverse_matrix(cz // 4), LANES),
    ]
    messages = 8 + 8 + 26 + 12 + nx - 1 + ny - 1
    vmem = lambda *s: pltpu.VMEM(s, f32)
    scratch = [
        vmem(cx, 2, cy + 2 * PAD, LANES), vmem(2, 2, cy + 2 * PAD, LANES), vmem(2, 2, cy, LANES),
        vmem(hx, 2, cy + 2 * PAD, LANES), vmem(hx, 2, cy + 2 * PAD, LANES),
        *[vmem(hx + 1, 2, hy + PAD, LANES) for _ in range(4)],
        vmem(hx, hy + 2 * PAD, LANES), vmem(2, hy + 2 * PAD, LANES), vmem(2, hy, LANES),
        vmem(qx, hy + 2 * PAD, LANES), vmem(qx, hy + 2 * PAD, LANES),
        vmem(qx + 6, qy + 2 * PAD, LANES),
        *[vmem(qx + 2, qy + 2 * PAD, LANES) for _ in range(3)],
        vmem(n3, qy + 2 * PAD, LANES), vmem(n3, qy + 2 * PAD, LANES),
        vmem(qx + 2, qy + 2 * PAD, LANES),
        vmem(hx + 2, 2 * (qy + 2 * PAD), LANES),
        vmem(cx, 2, hy + PAD, LANES), vmem(cx, 2, hy + PAD, LANES),
        vmem(cx, 2, cy, LANES), vmem(cx, cy, cz),
        vmem(nx, PAD, LANES), vmem(ny, PAD, LANES), vmem(PAD, LANES),
        pltpu.SemaphoreType.DMA((messages,)), pltpu.SemaphoreType.DMA((messages,)),
        pltpu.SemaphoreType.DMA((2,)), pltpu.SemaphoreType.DMA((cx // 8,)),
    ]
    return pl.pallas_call(
        functools.partial(kernel, (cx, cy, cz), count, nx, ny),
        out_shape=jax.ShapeDtypeStruct(volume.shape, f32),
        in_specs=[pl.BlockSpec(memory_space=pl.ANY)]
        + [pl.BlockSpec(memory_space=pltpu.VMEM)] * 6,
        out_specs=pl.BlockSpec(memory_space=pl.ANY),
        scratch_shapes=scratch,
        compiler_params=pltpu.CompilerParams(
            collective_id=0, has_side_effects=True, vmem_limit_bytes=56 * 1024 * 1024),
    )(volume, *[jnp.asarray(w) for w in weights])


def solution(mesh):
    spec = P("gx", "gy", None)
    body = functools.partial(on_device, mesh.shape["gx"], mesh.shape["gy"])
    return jax.shard_map(body, mesh=mesh, in_specs=(spec,), out_specs=spec, check_vma=False)
```

```python
import functools
import math

import jax
import jax.numpy as jnp
import numpy as np
from jax import lax
from jax.experimental import pallas as pl
from jax.experimental.pallas import tpu as pltpu
from jax.sharding import PartitionSpec as P

ROOT3 = math.sqrt(3.0)
NEAR = math.sqrt(3.0) / 4.0
FAR = (math.sqrt(3.0) - 2.0) / 4.0
LOW = (math.sqrt(3.0) - 1.0) / math.sqrt(2.0)
HIGH = (math.sqrt(3.0) + 1.0) / math.sqrt(2.0)
LANES = 128
PAD = 8


def forward_matrix(size):
    lines = np.eye(size)
    even, odd = lines[:, 0::2], lines[:, 1::2]
    smooth = even + ROOT3 * odd
    detail = odd - NEAR * smooth - FAR * np.roll(smooth, 1, 1)
    smooth = smooth - np.roll(detail, -1, 1)
    return np.concatenate([LOW * smooth, HIGH * detail], 1)


def inverse_matrix(size):
    lines = np.eye(size)
    smooth, detail = lines[:, : size // 2] / LOW, lines[:, size // 2 :] / HIGH
    first = smooth + np.roll(detail, -1, 1)
    odd = detail + NEAR * first + FAR * np.roll(first, 1, 1)
    even = first - ROOT3 * odd
    return np.stack([even, odd], 2).reshape(size, size)


def halves(matrix, size):
    full = np.zeros((size, size))
    full[: matrix.shape[0], : matrix.shape[1]] = matrix
    high = full.astype(jnp.bfloat16)
    low = (full - high.astype(np.float64)).astype(jnp.bfloat16)
    return np.stack([high, low])


def times(values, w_ref):
    high = values.astype(jnp.bfloat16)
    low = (values - high.astype(jnp.float32)).astype(jnp.bfloat16)
    dot = functools.partial(jnp.dot, preferred_element_type=jnp.float32)
    return dot(high, w_ref[0]) + (dot(low, w_ref[0]) + dot(high, w_ref[1]))


def shrink(values, noise):
    return values - jnp.clip(values, -noise, noise)


def sums(even, odd):
    smooth = even + ROOT3 * odd
    return smooth, odd - NEAR * smooth


def undo(detail, first, before):
    odd = detail + NEAR * first + FAR * before
    return first - ROOT3 * odd, odd


def weave(even, odd):
    both = jnp.stack([even, odd], axis=1)
    return both.reshape((2 * even.shape[0],) + even.shape[1:])


def forward_rows(even, odd):
    axis = even.ndim - 2
    smooth, part = sums(even, odd)
    detail = part - FAR * pltpu.roll(smooth, 1, axis)
    return HIGH * detail, LOW * (smooth - pltpu.roll(detail, even.shape[axis] - 1, axis))


def kernel(shape, count_all, nx, ny, vol, w1, w2, w3, v1, v2, v3, out,
           e1, hx1, sx1, hy1, sy1, hc1, sc1, xd1, xs1, s1s, s1d, d1s, d1d,
           e2, ht2, st2, xd2, xs2, ss, sd, ds, dd, ep3, t3d, t3s, r2, r1,
           p1s, p1d, o1, ob, part, total, send, recv, lsem, osem):
    cx, cy, cz = shape
    hx, hy, qx, qy = cx // 2, cy // 2, cx // 4, cy // 4
    ix, iy = lax.axis_index("gx"), lax.axis_index("gy")

    def device(dx, dy):
        return (lax.rem(ix + dx + nx, nx), lax.rem(iy + dy + ny, ny))

    loads = [
        pltpu.make_async_copy(
            vol.at[:, :, pl.ds(h * LANES, LANES)],
            e1.at[:, h, pl.ds(PAD, cy), :], lsem.at[h])
        for h in range(2)
    ]
    for c in loads:
        c.start()

    greet = [(dx, dy) for dx in (-1, 0, 1) for dy in (-1, 0, 1) if dx or dy]
    greet += [(dx, 0) for dx in range(2, nx - 1)] + [(0, dy) for dy in range(2, ny - 1)]
    barrier = pltpu.get_barrier_semaphore()
    for d in greet:
        pl.semaphore_signal(barrier, inc=1, device_id=device(*d),
                            device_id_type=pl.DeviceIdType.MESH)

    slot = [0]
    started = []

    def post(src, dst, dx, dy):
        n = slot[0]
        slot[0] += 1
        c = pltpu.make_async_remote_copy(
            src_ref=src, dst_ref=dst, send_sem=send.at[n], recv_sem=recv.at[n],
            device_id=device(dx, dy), device_id_type=pl.DeviceIdType.MESH)
        c.start()
        started.append(c)
        return c

    for c in loads:
        c.wait()

    top = PAD + cy
    sx1[1] = sums(e1[0, :, PAD:top], e1[1, :, PAD:top])[1]
    sy1[1] = sums(e1[:, :, PAD : PAD + 1], e1[:, :, PAD + 1 : PAD + 2])[1]
    sx1[0] = sums(e1[cx - 2, :, PAD:top], e1[cx - 1, :, PAD:top])[0]
    sy1[0] = sums(e1[:, :, top - 2 : top - 1], e1[:, :, top - 1 : top])[0]
    for x in range(2):
        sc1[x, 1] = sums(sx1[x, :, 0:1], sx1[x, :, 1:2])[1]
        sc1[x, 0] = sums(sx1[x, :, cy - 2 : cy - 1], sx1[x, :, cy - 1 : cy])[0]
    pl.semaphore_wait(barrier, len(greet))
    step = (1, -1)
    post_x = lambda x: post(sx1.at[x], hx1.at[x, :, pl.ds(PAD, cy), :], step[x], 0)
    post_y = lambda y: post(sy1.at[y], hy1.at[y], 0, step[y])
    post_c = lambda x, y: post(sc1.at[x, y], hc1.at[x, y], step[x], step[y])
    now1 = [post_c(1, 1), post_x(1), post_y(1)]
    later1 = [post_c(0, 1), post_c(1, 0), post_c(0, 0), post_x(0), post_y(0)]

    def place(ref, rows, side):
        if side == 0:
            ref[..., PAD - 2 : PAD - 1, :] = rows
            ref[..., PAD - 1 : PAD, :] = jnp.zeros_like(rows)
        else:
            ref[..., top : top + 1, :] = -ROOT3 * rows
            ref[..., top + 1 : top + 2, :] = rows

    def pair1(n):
        return sums(e1[2 * n], e1[2 * n + 1])

    for c in now1:
        c.wait_recv()
    place(e1, hy1[1], 1)
    place(hx1.at[1], hc1[1, 1], 1)

    def lift1(n, carry):
        smooth, part_n = pair1(n)
        before, _ = pair1(n - 1)
        detail = part_n - FAR * before
        xd1[n] = HIGH * detail
        xs1[n] = LOW * (before - detail)
        return carry

    lax.fori_loop(1, hx, lift1, 0)
    edge, _ = pair1(hx - 1)
    edge_d = hx1[1] - FAR * edge
    xd1[hx] = HIGH * edge_d
    xs1[hx] = LOW * (edge - edge_d)

    def coarse1(n, carry):
        for h in range(2):
            load = lambda start: xs1[n, h, pl.ds(start, hy, stride=2), :]
            s0, _ = sums(load(PAD), load(PAD + 1))
            _, tp = sums(load(PAD + 2), load(PAD + 3))
            s1s[n, h, PAD : PAD + hy] = LOW * (s0 - (tp - FAR * s0))
        return carry

    lax.fori_loop(1, hx + 1, coarse1, 0)

    def lines(ref, xs, ys):
        n = (xs.stop - xs.start) * (ys.stop - ys.start)
        return jnp.concatenate([ref[xs, h, ys].reshape(n, LANES) for h in range(2)], axis=1)

    chunk = hx // 2
    for i in range(2):
        rows = lines(s1s, slice(1 + i * chunk, 1 + (i + 1) * chunk), slice(PAD, PAD + hy))
        e2[4 + i * chunk : 4 + (i + 1) * chunk, PAD : PAD + hy] = times(
            rows, w1.at[:, :, 0:LANES]).reshape(chunk, hy, LANES)

    st2[...] = sums(e2[4, PAD : PAD + hy], e2[5, PAD : PAD + hy])[1]
    y_own, y_low, y_high = pl.ds(PAD, hy), pl.ds(0, PAD), pl.ds(PAD + hy, PAD)
    y_first, y_last = pl.ds(PAD, PAD), pl.ds(hy, PAD)
    own2, from2, to2 = pl.ds(4, hx), pl.ds(hx, 4), pl.ds(0, 4)
    now2 = [
        post(st2, ht2.at[y_own, :], -1, 0),
        post(e2.at[own2, y_first, :], e2.at[own2, y_high, :], 0, -1),
        post(st2.at[pl.ds(0, PAD), :], ht2.at[y_high, :], -1, -1),
    ]
    later2 = [
        post(e2.at[own2, y_last, :], e2.at[own2, y_low, :], 0, 1),
        post(e2.at[from2, y_own, :], e2.at[to2, y_own, :], 1, 0),
        post(e2.at[from2, y_last, :], e2.at[to2, y_low, :], 1, 1),
        post(e2.at[from2, y_first, :], e2.at[to2, y_high, :], 1, -1),
        post(st2.at[pl.ds(hy - PAD, PAD), :], ht2.at[y_low, :], -1, 1),
    ]

    for c in later1:
        c.wait_recv()
    place(e1, hy1[0], 0)
    place(hx1.at[1], hc1[1, 0], 0)
    place(hx1.at[0], hc1[0, 0], 0)
    place(hx1.at[0], hc1[0, 1], 1)
    first_s, first_t = pair1(0)
    first_d = first_t - FAR * hx1[0]
    xd1[0] = HIGH * first_d
    xs1[0] = LOW * (hx1[0] - first_d)
    low = slice(PAD - 2, PAD)

    def low1(n, carry):
        def pair(n):
            return sums(e1[2 * n, :, low], e1[2 * n + 1, :, low])
        _, part_n = pair(n)
        before, _ = pair(n - 1)
        detail = part_n - FAR * before
        xd1[n, :, low] = HIGH * detail
        xs1[n, :, low] = LOW * (before - detail)
        return carry

    lax.fori_loop(1, hx, low1, 0)
    edge, _ = sums(e1[cx - 2, :, low], e1[cx - 1, :, low])
    edge_d = hx1[1, :, low] - FAR * edge
    xd1[hx, :, low] = HIGH * edge_d
    xs1[hx, :, low] = LOW * (edge - edge_d)

    def cols1(n, carry):
        for h in range(2):
            for src, det, smo in ((xd1, d1d, d1s), (xs1, s1d, s1s)):
                load = lambda start: src[n, h, pl.ds(start, hy + 1, stride=2), :]
                s0, t0 = sums(load(PAD), load(PAD + 1))
                sm, _ = sums(load(PAD - 2), load(PAD - 1))
                d = t0 - FAR * sm
                det[n, h, 0 : hy + 1] = HIGH * d
                smo[n, h, PAD - 1 : PAD + hy] = LOW * (sm - d)
        return carry

    lax.fori_loop(0, hx + 1, cols1, 0)

    magnitude = jnp.zeros((PAD, LANES), jnp.float32)
    rows1 = hy + PAD
    for ref in (d1d, d1s, s1d, s1s):
        for lo, hi in ((0, chunk), (chunk, hx + 1)):
            rows = lines(ref, slice(lo, hi), slice(0, rows1))
            if ref is s1s:
                ref[lo:hi, 1] = times(rows, w1.at[:, :, LANES : 2 * LANES]).reshape(
                    hi - lo, rows1, LANES)
                continue
            got = times(rows, w1)
            for h in range(2):
                ref[lo:hi, h] = got[:, h * LANES : (h + 1) * LANES].reshape(hi - lo, rows1, LANES)
            if ref is d1d:
                mine = got[:, LANES:].reshape(hi - lo, rows1, LANES)[: chunk, :hy]
                magnitude = magnitude + jnp.sum(
                    jnp.abs(mine).reshape(chunk * hy // PAD, PAD, LANES), axis=0)
        if ref is d1d:
            part[0] = magnitude
            sums_x = [post(part.at[0], part.at[k], k, 0) for k in range(1, nx)]

    for c in now2:
        c.wait_recv()
    x2, yrows, pairs = qx + 2, qy + 2 * PAD, hy // 2 + PAD

    def lift2(rows):
        def step(n, carry):
            before, _ = sums(e2[2 * n, rows], e2[2 * n + 1, rows])
            _, part_n = sums(e2[2 * n + 2, rows], e2[2 * n + 3, rows])
            detail = part_n - FAR * before
            xd2[n, rows] = HIGH * detail
            xs2[n, rows] = LOW * (before - detail)
            return carry
        return step

    def last2(rows):
        before, _ = sums(e2[2 * x2 - 2, rows], e2[2 * x2 - 1, rows])
        detail = ht2[rows] - FAR * before
        xd2[x2 - 1, rows] = HIGH * detail
        xs2[x2 - 1, rows] = LOW * (before - detail)

    above, every = slice(PAD, hy + 2 * PAD), slice(0, hy + 2 * PAD)
    lax.fori_loop(2, x2 - 1, lift2(above), 0)
    last2(above)
    load2 = lambda start: xs2[2:x2, pl.ds(start, qy, stride=2), :]
    s0, _ = sums(load2(PAD), load2(PAD + 1))
    _, tp = sums(load2(PAD + 2), load2(PAD + 3))
    smooth2 = LOW * (s0 - (tp - FAR * s0))
    coarse2 = times(smooth2.reshape(qx * qy, LANES), w2)
    coarse2 = coarse2.reshape(qx // 2, 2, qy, LANES)
    lane = lax.broadcasted_iota(jnp.int32, (qx // 2, qy, LANES), 2)
    half = LANES // 2
    packed = jnp.where(lane < half, coarse2[:, 0], pltpu.roll(coarse2[:, 1], half, 2))
    ep3[2 : 2 + qx // 2, PAD : PAD + qy] = packed

    n_own = qx // 2
    own3 = pl.ds(2, n_own)
    z_own, z_low, z_high = pl.ds(PAD, qy), pl.ds(0, PAD), pl.ds(PAD + qy, PAD)
    z_first, z_last = pl.ds(PAD, PAD), pl.ds(qy, PAD)
    round3 = []
    for dx, xs, xd in ((1, pl.ds(n_own, 2), pl.ds(0, 2)),
                       (-1, pl.ds(2, 1), pl.ds(2 + n_own, 1)), (0, own3, own3)):
        for dy, ys, yd in ((0, z_own, z_own), (1, z_last, z_low), (-1, z_first, z_high)):
            if dx or dy:
                round3.append(post(ep3.at[xs, ys, :], ep3.at[xd, yd, :], dx, dy))

    for c in sums_x:
        c.wait_recv()
    acc = part[0]
    for k in range(1, nx):
        acc = acc + part[k]
    total[0] = acc
    sums_y = [post(total.at[0], total.at[k], 0, k) for k in range(1, ny)]

    for c in later2:
        c.wait_recv()
    lax.fori_loop(0, x2 - 1, lift2(every), 0)
    last2(every)

    def rows2(src, at):
        return forward_rows(src[at, pl.ds(0, pairs, stride=2), :],
                            src[at, pl.ds(1, pairs, stride=2), :])

    for src, det, smo in ((xd2, dd, ds), (xs2, sd, ss)):
        for band, dst in zip(rows2(src, slice(0, x2)), (det, smo)):
            dst[:, PAD // 2 : PAD // 2 + pairs] = times(
                band.reshape(x2 * pairs, LANES), w2).reshape(x2, pairs, LANES)

    for c in round3:
        c.wait_recv()
    low_s, low_t = [], []
    for n in range(n_own + 3):
        s, t = sums(ep3[n], pltpu.roll(ep3[n], half, 1))
        low_s.append(s)
        low_t.append(t)
    n3 = n_own + 2
    for n in range(n3):
        detail = low_t[n + 1] - FAR * low_s[n]
        t3d[n] = HIGH * detail
        t3s[n] = LOW * (low_s[n] - detail)
    h3 = qy // 2 + PAD
    bands = []
    for src in (t3d, t3s):
        bands += forward_rows(src[:, pl.ds(0, h3, stride=2), :], src[:, pl.ds(1, h3, stride=2), :])
    for i, band in enumerate(bands):
        bands[i] = times(band.reshape(n3 * h3, LANES), w3).reshape(n3, h3, LANES)

    for c in sums_y:
        c.wait_recv()
    acc = total[0]
    for k in range(1, ny):
        acc = acc + total[k]
    noise = jnp.sum(acc, axis=(0, 1), keepdims=True) * (math.sqrt(math.pi / 2.0) / count_all)

    lane3 = lax.broadcasted_iota(jnp.int32, (n3, h3, LANES), 2)
    noise3 = noise.reshape(1, 1, 1)
    b_dd, b_ds, b_sd = (shrink(b, noise3) for b in bands[:3])
    b_ss = jnp.where(lane3 < cz // 8, bands[3], shrink(bands[3], noise3))

    def inverse_x(det, smo):
        det, smo = det * (1.0 / HIGH), smo * (1.0 / LOW)
        one = smo + det
        even, odd = undo(det[:-1], one[1:], one[:-1])
        return weave(even, odd)

    y_d = inverse_x(b_dd, b_sd) * (1.0 / HIGH)
    y_s = inverse_x(b_ds, b_ss) * (1.0 / LOW)
    one = y_s + pltpu.roll(y_d, h3 - 1, 1)
    even, odd = undo(y_d, one, pltpu.roll(one, 1, 1))
    r2[:, pl.ds(0, h3, stride=2), :] = even
    r2[:, pl.ds(1, h3, stride=2), :] = odd
    back = times(r2[...].reshape(x2 * yrows, LANES), v3).reshape(x2, yrows, LANES)

    lane2 = lax.broadcasted_iota(jnp.int32, (x2, yrows, LANES), 2)
    ss[...] = jnp.where(lane2 < cz // 4, back, shrink(ss[...], noise3))

    def inv2(n, carry):
        def one_x(n):
            d_d = shrink(dd[n], noise) * (1.0 / HIGH)
            d_s = shrink(ds[n], noise) * (1.0 / HIGH)
            s_d = shrink(sd[n], noise) * (1.0 / LOW)
            s_s = ss[n] * (1.0 / LOW)
            return d_d, d_s, s_d + d_d, s_s + d_s

        d_d, d_s, b_d, b_s = one_x(n)
        _, _, f_d, f_s = one_x(n + 1)
        pair_d = undo(d_d, f_d, b_d)
        pair_s = undo(d_s, f_s, b_s)
        for i in range(2):
            y_d, y_s = pair_d[i] * (1.0 / HIGH), pair_s[i] * (1.0 / LOW)
            one = y_s + pltpu.roll(y_d, yrows - 1, 0)
            even, odd = undo(y_d, one, pltpu.roll(one, 1, 0))
            r1[2 * n + i, pl.ds(0, yrows, stride=2), :] = even
            r1[2 * n + i, pl.ds(1, yrows, stride=2), :] = odd
        return carry

    lax.fori_loop(0, qx + 1, inv2, 0)
    x1, y1 = hx + 2, hy + PAD
    back = times(r1[:, PAD : PAD + y1].reshape(x1 * y1, LANES), v2).reshape(x1, y1, LANES)
    s1s[:, 0] = back[1:]

    def inv1(n, carry):
        for h in range(2):
            for det, smo, dst in ((d1d, s1d, p1d), (d1s, s1s, p1s)):
                plain = smo is s1s and h == 0

                def one_x(n):
                    d = shrink(det[n, h], noise) * (1.0 / HIGH)
                    s = smo[n, h] if plain else shrink(smo[n, h], noise)
                    return d, s * (1.0 / LOW) + d

                d, before = one_x(n)
                _, one = one_x(n + 1)
                even, odd = undo(d, one, before)
                dst[2 * n, h] = even
                dst[2 * n + 1, h] = odd
        return carry

    lax.fori_loop(0, hx, inv1, 0)

    def inv1_y(n, carry):
        for h in range(2):
            y_d = p1d[n, h, 0:hy] * (1.0 / HIGH)
            y_n = p1d[n, h, 1 : hy + 1] * (1.0 / HIGH)
            s = p1s[n, h, PAD : PAD + hy] * (1.0 / LOW)
            s_b = p1s[n, h, PAD - 1 : PAD - 1 + hy] * (1.0 / LOW)
            even, odd = undo(y_d, s + y_n, s_b + y_d)
            o1[n, h, pl.ds(0, hy, stride=2), :] = even
            o1[n, h, pl.ds(1, hy, stride=2), :] = odd
        return carry

    lax.fori_loop(0, cx, inv1_y, 0)
    layers = 8
    outs = []
    for i in range(cx // layers):
        xs = slice(i * layers, (i + 1) * layers)
        rows = jnp.concatenate(
            [o1[xs, h].reshape(layers * cy, LANES) for h in range(2)], axis=1)
        ob[xs] = times(rows, v1).reshape(layers, cy, cz)
        c = pltpu.make_async_copy(ob.at[xs], out.at[xs], osem.at[i])
        c.start()
        outs.append(c)
    for c in outs:
        c.wait()
    for c in started:
        c.wait_send()


def on_device(nx, ny, volume):
    cx, cy, cz = volume.shape
    hx, hy, qx, qy = cx // 2, cy // 2, cx // 4, cy // 4
    n3, h3 = qx // 2 + 2, qy // 2 + PAD
    f32 = jnp.float32
    count = cx * nx * cy * ny * cz // 8
    weights = [
        halves(forward_matrix(cz), cz), halves(forward_matrix(cz // 2), LANES),
        halves(forward_matrix(cz // 4), LANES), halves(inverse_matrix(cz), cz),
        halves(inverse_matrix(cz // 2), LANES), halves(inverse_matrix(cz // 4), LANES),
    ]
    messages = 24 + nx - 1 + ny - 1
    vmem = lambda *s: pltpu.VMEM(s, f32)
    ey, ey2, ey3 = cy + 2 * PAD, hy + 2 * PAD, qy + 2 * PAD
    scratch = [
        vmem(cx, 2, ey, LANES), vmem(2, 2, ey, LANES), vmem(2, 2, cy, LANES),
        vmem(2, cx, 2, 1, LANES), vmem(2, cx, 2, 1, LANES),
        vmem(2, 2, 2, 1, LANES), vmem(2, 2, 2, 1, LANES),
        vmem(hx + 1, 2, ey, LANES), vmem(hx + 1, 2, ey, LANES),
        *[vmem(hx + 1, 2, hy + PAD, LANES) for _ in range(4)],
        vmem(hx + 4, ey2, LANES), vmem(ey2, LANES), vmem(hy, LANES),
        vmem(qx + 2, ey2, LANES), vmem(qx + 2, ey2, LANES),
        *[vmem(qx + 2, ey3, LANES) for _ in range(4)],
        vmem(qx // 2 + 3, ey3, LANES),
        vmem(n3, ey3, LANES), vmem(n3, ey3, LANES),
        vmem(qx + 2, ey3, LANES),
        vmem(hx + 2, 2 * ey3, LANES),
        vmem(cx, 2, hy + PAD, LANES), vmem(cx, 2, hy + PAD, LANES),
        vmem(cx, 2, cy, LANES), vmem(cx, cy, cz),
        vmem(nx, PAD, LANES), vmem(ny, PAD, LANES),
        pltpu.SemaphoreType.DMA((messages,)), pltpu.SemaphoreType.DMA((messages,)),
        pltpu.SemaphoreType.DMA((2,)), pltpu.SemaphoreType.DMA((cx // 8,)),
    ]
    return pl.pallas_call(
        functools.partial(kernel, (cx, cy, cz), count, nx, ny),
        out_shape=jax.ShapeDtypeStruct(volume.shape, f32),
        in_specs=[pl.BlockSpec(memory_space=pl.ANY)]
        + [pl.BlockSpec(memory_space=pltpu.VMEM)] * 6,
        out_specs=pl.BlockSpec(memory_space=pl.ANY),
        scratch_shapes=scratch,
        compiler_params=pltpu.CompilerParams(
            collective_id=0, has_side_effects=True, vmem_limit_bytes=56 * 1024 * 1024),
    )(volume, *[jnp.asarray(w) for w in weights])


def solution(mesh):
    spec = P("gx", "gy", None)
    body = functools.partial(on_device, mesh.shape["gx"], mesh.shape["gy"])
    return jax.shard_map(body, mesh=mesh, in_specs=(spec,), out_specs=spec, check_vma=False)
```

```python
import functools
import math

import jax
import jax.numpy as jnp
import numpy as np
from jax import lax
from jax.experimental import pallas as pl
from jax.experimental.pallas import tpu as pltpu
from jax.sharding import PartitionSpec as P

ROOT3 = math.sqrt(3.0)
NEAR = math.sqrt(3.0) / 4.0
FAR = (math.sqrt(3.0) - 2.0) / 4.0
LOW = (math.sqrt(3.0) - 1.0) / math.sqrt(2.0)
HIGH = (math.sqrt(3.0) + 1.0) / math.sqrt(2.0)
LANES = 128
PAD = 8


def forward_matrix(size):
    lines = np.eye(size)
    even, odd = lines[:, 0::2], lines[:, 1::2]
    smooth = even + ROOT3 * odd
    detail = odd - NEAR * smooth - FAR * np.roll(smooth, 1, 1)
    smooth = smooth - np.roll(detail, -1, 1)
    return np.concatenate([LOW * smooth, HIGH * detail], 1)


def inverse_matrix(size):
    lines = np.eye(size)
    smooth, detail = lines[:, : size // 2] / LOW, lines[:, size // 2 :] / HIGH
    first = smooth + np.roll(detail, -1, 1)
    odd = detail + NEAR * first + FAR * np.roll(first, 1, 1)
    even = first - ROOT3 * odd
    return np.stack([even, odd], 2).reshape(size, size)


def halves(matrix, size):
    full = np.zeros((size, size))
    full[: matrix.shape[0], : matrix.shape[1]] = matrix
    high = full.astype(jnp.bfloat16)
    low = (full - high.astype(np.float64)).astype(jnp.bfloat16)
    return np.stack([high, low])


def times(values, w_ref):
    high = values.astype(jnp.bfloat16)
    low = (values - high.astype(jnp.float32)).astype(jnp.bfloat16)
    dot = functools.partial(jnp.dot, preferred_element_type=jnp.float32)
    return dot(high, w_ref[0]) + (dot(low, w_ref[0]) + dot(high, w_ref[1]))


def shrink(values, noise):
    return values - jnp.clip(values, -noise, noise)


def sums(even, odd):
    smooth = even + ROOT3 * odd
    return smooth, odd - NEAR * smooth


def undo(detail, first, before):
    odd = detail + NEAR * first + FAR * before
    return first - ROOT3 * odd, odd


def weave(even, odd):
    both = jnp.stack([even, odd], axis=1)
    return both.reshape((2 * even.shape[0],) + even.shape[1:])


def forward_rows(even, odd):
    axis = even.ndim - 2
    smooth, part = sums(even, odd)
    detail = part - FAR * pltpu.roll(smooth, 1, axis)
    return HIGH * detail, LOW * (smooth - pltpu.roll(detail, even.shape[axis] - 1, axis))


def kernel(shape, count_all, nx, ny, vol, g1, g2, g3, g4, g5, g6, o1, v1,
           w1, w2, w3, v2, v3,
           e1, hx1, sx1, hy1, sy1, hc1, sc1, xd1, xs1, s1s, s1d, d1s, d1d,
           e2, ht2, st2, xd2, xs2, ss, sd, ds, dd, ep3, t3d, t3s, r2, r1,
           p1s, p1d, part, total, send, recv, lsem, wsem):
    cx, cy, cz = shape
    hx, hy, qx, qy = cx // 2, cy // 2, cx // 4, cy // 4
    ix, iy = lax.axis_index("gx"), lax.axis_index("gy")

    def device(dx, dy):
        return (lax.rem(ix + dx + nx, nx), lax.rem(iy + dy + ny, ny))

    loads = [
        pltpu.make_async_copy(
            vol.at[:, :, pl.ds(h * LANES, LANES)],
            e1.at[:, h, pl.ds(PAD, cy), :], lsem.at[h])
        for h in range(2)
    ]
    weights = [
        pltpu.make_async_copy(src, dst, wsem.at[i])
        for i, (src, dst) in enumerate(
            zip((g1, g2, g3, g4, g5, g6), (w1, w2, w3, v1, v2, v3)))
    ]
    for c in loads + weights:
        c.start()

    greet = [(dx, dy) for dx in (-1, 0, 1) for dy in (-1, 0, 1) if dx or dy]
    greet += [(dx, 0) for dx in range(2, nx - 1)] + [(0, dy) for dy in range(2, ny - 1)]
    barrier = pltpu.get_barrier_semaphore()
    for d in greet:
        pl.semaphore_signal(barrier, inc=1, device_id=device(*d),
                            device_id_type=pl.DeviceIdType.MESH)

    slot = [0]
    started = []

    def post(src, dst, dx, dy):
        n = slot[0]
        slot[0] += 1
        c = pltpu.make_async_remote_copy(
            src_ref=src, dst_ref=dst, send_sem=send.at[n], recv_sem=recv.at[n],
            device_id=device(dx, dy), device_id_type=pl.DeviceIdType.MESH)
        c.start()
        started.append(c)
        return c

    for c in loads:
        c.wait()

    top = PAD + cy
    sx1[1] = sums(e1[0, :, PAD:top], e1[1, :, PAD:top])[1]
    sy1[1] = sums(e1[:, :, PAD : PAD + 1], e1[:, :, PAD + 1 : PAD + 2])[1]
    sx1[0] = sums(e1[cx - 2, :, PAD:top], e1[cx - 1, :, PAD:top])[0]
    sy1[0] = sums(e1[:, :, top - 2 : top - 1], e1[:, :, top - 1 : top])[0]
    for x in range(2):
        sc1[x, 1] = sums(sx1[x, :, 0:1], sx1[x, :, 1:2])[1]
        sc1[x, 0] = sums(sx1[x, :, cy - 2 : cy - 1], sx1[x, :, cy - 1 : cy])[0]
    pl.semaphore_wait(barrier, len(greet))
    step = (1, -1)
    post_x = lambda x: post(sx1.at[x], hx1.at[x, :, pl.ds(PAD, cy), :], step[x], 0)
    post_y = lambda y: post(sy1.at[y], hy1.at[y], 0, step[y])
    post_c = lambda x, y: post(sc1.at[x, y], hc1.at[x, y], step[x], step[y])
    now1 = [post_c(1, 1), post_x(1), post_y(1)]
    later1 = [post_c(0, 1), post_c(1, 0), post_c(0, 0), post_x(0), post_y(0)]

    def place(ref, rows, side):
        if side == 0:
            ref[..., PAD - 2 : PAD - 1, :] = rows
            ref[..., PAD - 1 : PAD, :] = jnp.zeros_like(rows)
        else:
            ref[..., top : top + 1, :] = -ROOT3 * rows
            ref[..., top + 1 : top + 2, :] = rows

    def pair1(n):
        return sums(e1[2 * n], e1[2 * n + 1])

    for c in now1:
        c.wait_recv()
    place(e1, hy1[1], 1)
    place(hx1.at[1], hc1[1, 1], 1)

    def lift1(n, carry):
        smooth, part_n = pair1(n)
        before, _ = pair1(n - 1)
        detail = part_n - FAR * before
        xd1[n] = HIGH * detail
        xs1[n] = LOW * (before - detail)
        return carry

    lax.fori_loop(1, hx, lift1, 0)
    edge, _ = pair1(hx - 1)
    edge_d = hx1[1] - FAR * edge
    xd1[hx] = HIGH * edge_d
    xs1[hx] = LOW * (edge - edge_d)

    def coarse1(n, carry):
        for h in range(2):
            load = lambda start: xs1[n, h, pl.ds(start, hy, stride=2), :]
            s0, _ = sums(load(PAD), load(PAD + 1))
            _, tp = sums(load(PAD + 2), load(PAD + 3))
            s1s[n, h, PAD : PAD + hy] = LOW * (s0 - (tp - FAR * s0))
        return carry

    lax.fori_loop(1, hx + 1, coarse1, 0)
    for c in weights:
        c.wait()

    def lines(ref, xs, ys):
        n = (xs.stop - xs.start) * (ys.stop - ys.start)
        return jnp.concatenate([ref[xs, h, ys].reshape(n, LANES) for h in range(2)], axis=1)

    chunk = hx // 2
    for i in range(2):
        rows = lines(s1s, slice(1 + i * chunk, 1 + (i + 1) * chunk), slice(PAD, PAD + hy))
        e2[4 + i * chunk : 4 + (i + 1) * chunk, PAD : PAD + hy] = times(
            rows, w1.at[:, :, 0:LANES]).reshape(chunk, hy, LANES)

    st2[...] = sums(e2[4, PAD : PAD + hy], e2[5, PAD : PAD + hy])[1]
    y_own, y_low, y_high = pl.ds(PAD, hy), pl.ds(0, PAD), pl.ds(PAD + hy, PAD)
    y_first, y_last = pl.ds(PAD, PAD), pl.ds(hy, PAD)
    own2, from2, to2 = pl.ds(4, hx), pl.ds(hx, 4), pl.ds(0, 4)
    now2 = [
        post(st2, ht2.at[y_own, :], -1, 0),
        post(e2.at[own2, y_first, :], e2.at[own2, y_high, :], 0, -1),
        post(st2.at[pl.ds(0, PAD), :], ht2.at[y_high, :], -1, -1),
    ]
    later2 = [
        post(e2.at[own2, y_last, :], e2.at[own2, y_low, :], 0, 1),
        post(e2.at[from2, y_own, :], e2.at[to2, y_own, :], 1, 0),
        post(e2.at[from2, y_last, :], e2.at[to2, y_low, :], 1, 1),
        post(e2.at[from2, y_first, :], e2.at[to2, y_high, :], 1, -1),
        post(st2.at[pl.ds(hy - PAD, PAD), :], ht2.at[y_low, :], -1, 1),
    ]

    for c in later1:
        c.wait_recv()
    place(e1, hy1[0], 0)
    place(hx1.at[1], hc1[1, 0], 0)
    place(hx1.at[0], hc1[0, 0], 0)
    place(hx1.at[0], hc1[0, 1], 1)
    first_s, first_t = pair1(0)
    first_d = first_t - FAR * hx1[0]
    xd1[0] = HIGH * first_d
    xs1[0] = LOW * (hx1[0] - first_d)
    low = slice(PAD - 2, PAD)

    def low1(n, carry):
        def pair(n):
            return sums(e1[2 * n, :, low], e1[2 * n + 1, :, low])
        _, part_n = pair(n)
        before, _ = pair(n - 1)
        detail = part_n - FAR * before
        xd1[n, :, low] = HIGH * detail
        xs1[n, :, low] = LOW * (before - detail)
        return carry

    lax.fori_loop(1, hx, low1, 0)
    edge, _ = sums(e1[cx - 2, :, low], e1[cx - 1, :, low])
    edge_d = hx1[1, :, low] - FAR * edge
    xd1[hx, :, low] = HIGH * edge_d
    xs1[hx, :, low] = LOW * (edge - edge_d)

    def cols1(src, det, smo):
        def step(n, carry):
            for h in range(2):
                load = lambda start: src[n, h, pl.ds(start, hy + 1, stride=2), :]
                s0, t0 = sums(load(PAD), load(PAD + 1))
                sm, _ = sums(load(PAD - 2), load(PAD - 1))
                d = t0 - FAR * sm
                det[n, h, 0 : hy + 1] = HIGH * d
                smo[n, h, PAD - 1 : PAD + hy] = LOW * (sm - d)
            return carry

        lax.fori_loop(0, hx + 1, step, 0)

    rows1 = hy + PAD
    parts1 = ((0, chunk), (chunk, hx + 1))

    def depth1(ref):
        magnitude = jnp.zeros((PAD, LANES), jnp.float32)
        for lo, hi in parts1:
            rows = lines(ref, slice(lo, hi), slice(0, rows1))
            if ref is s1s:
                ref[lo:hi, 1] = times(rows, w1.at[:, :, LANES : 2 * LANES]).reshape(
                    hi - lo, rows1, LANES)
                continue
            got = times(rows, w1)
            for h in range(2):
                ref[lo:hi, h] = got[:, h * LANES : (h + 1) * LANES].reshape(hi - lo, rows1, LANES)
            if ref is d1d:
                mine = got[:, LANES:].reshape(hi - lo, rows1, LANES)[:chunk, :hy]
                magnitude = magnitude + jnp.sum(
                    jnp.abs(mine).reshape(chunk * hy // PAD, PAD, LANES), axis=0)
        return magnitude

    cols1(xd1, d1d, d1s)
    part[0] = depth1(d1d)
    sums_x = [post(part.at[0], part.at[k], k, 0) for k in range(1, nx)]

    for c in now2:
        c.wait_recv()
    x2, yrows, pairs = qx + 2, qy + 2 * PAD, hy // 2 + PAD

    def lift2(rows):
        def step(n, carry):
            before, _ = sums(e2[2 * n, rows], e2[2 * n + 1, rows])
            _, part_n = sums(e2[2 * n + 2, rows], e2[2 * n + 3, rows])
            detail = part_n - FAR * before
            xd2[n, rows] = HIGH * detail
            xs2[n, rows] = LOW * (before - detail)
            return carry
        return step

    def last2(rows):
        before, _ = sums(e2[2 * x2 - 2, rows], e2[2 * x2 - 1, rows])
        detail = ht2[rows] - FAR * before
        xd2[x2 - 1, rows] = HIGH * detail
        xs2[x2 - 1, rows] = LOW * (before - detail)

    above, every = slice(PAD, hy + 2 * PAD), slice(0, hy + 2 * PAD)
    lax.fori_loop(2, x2 - 1, lift2(above), 0)
    last2(above)
    load2 = lambda start: xs2[2:x2, pl.ds(start, qy, stride=2), :]
    s0, _ = sums(load2(PAD), load2(PAD + 1))
    _, tp = sums(load2(PAD + 2), load2(PAD + 3))
    smooth2 = LOW * (s0 - (tp - FAR * s0))
    coarse2 = times(smooth2.reshape(qx * qy, LANES), w2)
    coarse2 = coarse2.reshape(qx // 2, 2, qy, LANES)
    lane = lax.broadcasted_iota(jnp.int32, (qx // 2, qy, LANES), 2)
    half = LANES // 2
    packed = jnp.where(lane < half, coarse2[:, 0], pltpu.roll(coarse2[:, 1], half, 2))
    ep3[2 : 2 + qx // 2, PAD : PAD + qy] = packed

    n_own = qx // 2
    own3 = pl.ds(2, n_own)
    z_own, z_low, z_high = pl.ds(PAD, qy), pl.ds(0, PAD), pl.ds(PAD + qy, PAD)
    z_first, z_last = pl.ds(PAD, PAD), pl.ds(qy, PAD)
    round3 = []
    for dx, xs, xd in ((1, pl.ds(n_own, 2), pl.ds(0, 2)),
                       (-1, pl.ds(2, 1), pl.ds(2 + n_own, 1)), (0, own3, own3)):
        for dy, ys, yd in ((0, z_own, z_own), (1, z_last, z_low), (-1, z_first, z_high)):
            if dx or dy:
                round3.append(post(ep3.at[xs, ys, :], ep3.at[xd, yd, :], dx, dy))

    cols1(xs1, s1d, s1s)
    depth1(d1s)

    for c in sums_x:
        c.wait_recv()
    acc = part[0]
    for k in range(1, nx):
        acc = acc + part[k]
    total[0] = acc
    sums_y = [post(total.at[0], total.at[k], 0, k) for k in range(1, ny)]

    depth1(s1d)
    depth1(s1s)

    for c in later2:
        c.wait_recv()
    lax.fori_loop(0, x2 - 1, lift2(every), 0)
    last2(every)

    def rows2(src, at):
        return forward_rows(src[at, pl.ds(0, pairs, stride=2), :],
                            src[at, pl.ds(1, pairs, stride=2), :])

    for src, det, smo in ((xd2, dd, ds), (xs2, sd, ss)):
        for band, dst in zip(rows2(src, slice(0, x2)), (det, smo)):
            dst[:, PAD // 2 : PAD // 2 + pairs] = times(
                band.reshape(x2 * pairs, LANES), w2).reshape(x2, pairs, LANES)

    for c in round3:
        c.wait_recv()
    low_s, low_t = [], []
    for n in range(n_own + 3):
        s, t = sums(ep3[n], pltpu.roll(ep3[n], half, 1))
        low_s.append(s)
        low_t.append(t)
    n3 = n_own + 2
    for n in range(n3):
        detail = low_t[n + 1] - FAR * low_s[n]
        t3d[n] = HIGH * detail
        t3s[n] = LOW * (low_s[n] - detail)
    h3 = qy // 2 + PAD
    bands = []
    for src in (t3d, t3s):
        bands += forward_rows(src[:, pl.ds(0, h3, stride=2), :], src[:, pl.ds(1, h3, stride=2), :])
    for i, band in enumerate(bands):
        bands[i] = times(band.reshape(n3 * h3, LANES), w3).reshape(n3, h3, LANES)

    for c in sums_y:
        c.wait_recv()
    acc = total[0]
    for k in range(1, ny):
        acc = acc + total[k]
    noise = jnp.sum(acc, axis=(0, 1), keepdims=True) * (math.sqrt(math.pi / 2.0) / count_all)

    lane3 = lax.broadcasted_iota(jnp.int32, (n3, h3, LANES), 2)
    noise3 = noise.reshape(1, 1, 1)
    b_dd, b_ds, b_sd = (shrink(b, noise3) for b in bands[:3])
    b_ss = jnp.where(lane3 < cz // 8, bands[3], shrink(bands[3], noise3))

    def inverse_x(det, smo):
        det, smo = det * (1.0 / HIGH), smo * (1.0 / LOW)
        one = smo + det
        even, odd = undo(det[:-1], one[1:], one[:-1])
        return weave(even, odd)

    y_d = inverse_x(b_dd, b_sd) * (1.0 / HIGH)
    y_s = inverse_x(b_ds, b_ss) * (1.0 / LOW)
    one = y_s + pltpu.roll(y_d, h3 - 1, 1)
    even, odd = undo(y_d, one, pltpu.roll(one, 1, 1))
    r2[:, pl.ds(0, h3, stride=2), :] = even
    r2[:, pl.ds(1, h3, stride=2), :] = odd
    back = times(r2[...].reshape(x2 * yrows, LANES), v3).reshape(x2, yrows, LANES)

    lane2 = lax.broadcasted_iota(jnp.int32, (x2, yrows, LANES), 2)
    ss[...] = jnp.where(lane2 < cz // 4, back, shrink(ss[...], noise3))

    def inv2(n, carry):
        def one_x(n):
            d_d = shrink(dd[n], noise) * (1.0 / HIGH)
            d_s = shrink(ds[n], noise) * (1.0 / HIGH)
            s_d = shrink(sd[n], noise) * (1.0 / LOW)
            s_s = ss[n] * (1.0 / LOW)
            return d_d, d_s, s_d + d_d, s_s + d_s

        d_d, d_s, b_d, b_s = one_x(n)
        _, _, f_d, f_s = one_x(n + 1)
        pair_d = undo(d_d, f_d, b_d)
        pair_s = undo(d_s, f_s, b_s)
        for i in range(2):
            y_d, y_s = pair_d[i] * (1.0 / HIGH), pair_s[i] * (1.0 / LOW)
            one = y_s + pltpu.roll(y_d, yrows - 1, 0)
            even, odd = undo(y_d, one, pltpu.roll(one, 1, 0))
            r1[2 * n + i, pl.ds(0, yrows, stride=2), :] = even
            r1[2 * n + i, pl.ds(1, yrows, stride=2), :] = odd
        return carry

    lax.fori_loop(0, qx + 1, inv2, 0)
    x1, y1 = hx + 2, hy + PAD
    back = times(r1[:, PAD : PAD + y1].reshape(x1 * y1, LANES), v2).reshape(x1, y1, LANES)
    s1s[:, 0] = back[1:]

    def inv1(n, carry):
        for h in range(2):
            for det, smo, dst in ((d1d, s1d, p1d), (d1s, s1s, p1s)):
                plain = smo is s1s and h == 0

                def one_x(n):
                    d = shrink(det[n, h], noise) * (1.0 / HIGH)
                    s = smo[n, h] if plain else shrink(smo[n, h], noise)
                    return d, s * (1.0 / LOW) + d

                d, before = one_x(n)
                _, one = one_x(n + 1)
                even, odd = undo(d, one, before)
                dst[2 * n, h] = even
                dst[2 * n + 1, h] = odd
        return carry

    lax.fori_loop(0, hx, inv1, 0)

    def inv1_y(n, carry):
        for h in range(2):
            y_d = p1d[n, h, 0:hy] * (1.0 / HIGH)
            y_n = p1d[n, h, 1 : hy + 1] * (1.0 / HIGH)
            s = p1s[n, h, PAD : PAD + hy] * (1.0 / LOW)
            s_b = p1s[n, h, PAD - 1 : PAD - 1 + hy] * (1.0 / LOW)
            even, odd = undo(y_d, s + y_n, s_b + y_d)
            o1[n, h, pl.ds(0, hy, stride=2), :] = even
            o1[n, h, pl.ds(1, hy, stride=2), :] = odd
        return carry

    lax.fori_loop(0, cx, inv1_y, 0)
    for c in started:
        c.wait_send()


def finish(rows_in, v1, out, ob, osem):
    cx, cy, cz = out.shape
    layers = 8
    outs = []
    for i in range(cx // layers):
        xs = slice(i * layers, (i + 1) * layers)
        rows = jnp.concatenate(
            [rows_in[xs, h].reshape(layers * cy, LANES) for h in range(2)], axis=1)
        ob[xs] = times(rows, v1).reshape(layers, cy, cz)
        c = pltpu.make_async_copy(ob.at[xs], out.at[xs], osem.at[i])
        c.start()
        outs.append(c)
    for c in outs:
        c.wait()


def on_device(nx, ny, volume):
    cx, cy, cz = volume.shape
    hx, hy, qx, qy = cx // 2, cy // 2, cx // 4, cy // 4
    n3, h3 = qx // 2 + 2, qy // 2 + PAD
    f32 = jnp.float32
    count = cx * nx * cy * ny * cz // 8
    weights = [
        halves(forward_matrix(cz), cz), halves(forward_matrix(cz // 2), LANES),
        halves(forward_matrix(cz // 4), LANES), halves(inverse_matrix(cz), cz),
        halves(inverse_matrix(cz // 2), LANES), halves(inverse_matrix(cz // 4), LANES),
    ]
    messages = 24 + nx - 1 + ny - 1
    vmem = lambda *s: pltpu.VMEM(s, f32)
    ey, ey2, ey3 = cy + 2 * PAD, hy + 2 * PAD, qy + 2 * PAD
    wide = lambda n: pltpu.VMEM((2, n, n), jnp.bfloat16)
    scratch = [
        wide(cz), wide(LANES), wide(LANES), wide(LANES), wide(LANES),
        vmem(cx, 2, ey, LANES), vmem(2, 2, ey, LANES), vmem(2, 2, cy, LANES),
        vmem(2, cx, 2, 1, LANES), vmem(2, cx, 2, 1, LANES),
        vmem(2, 2, 2, 1, LANES), vmem(2, 2, 2, 1, LANES),
        vmem(hx + 1, 2, ey, LANES), vmem(hx + 1, 2, ey, LANES),
        *[vmem(hx + 1, 2, hy + PAD, LANES) for _ in range(4)],
        vmem(hx + 4, ey2, LANES), vmem(ey2, LANES), vmem(hy, LANES),
        vmem(qx + 2, ey2, LANES), vmem(qx + 2, ey2, LANES),
        *[vmem(qx + 2, ey3, LANES) for _ in range(4)],
        vmem(qx // 2 + 3, ey3, LANES),
        vmem(n3, ey3, LANES), vmem(n3, ey3, LANES),
        vmem(qx + 2, ey3, LANES),
        vmem(hx + 2, 2 * ey3, LANES),
        vmem(cx, 2, hy + PAD, LANES), vmem(cx, 2, hy + PAD, LANES),
        vmem(nx, PAD, LANES), vmem(ny, PAD, LANES),
        pltpu.SemaphoreType.DMA((messages,)), pltpu.SemaphoreType.DMA((messages,)),
        pltpu.SemaphoreType.DMA((2,)), pltpu.SemaphoreType.DMA((6,)),
    ]
    near = pl.BlockSpec(memory_space=pltpu.VMEM)
    rows, v1 = pl.pallas_call(
        functools.partial(kernel, (cx, cy, cz), count, nx, ny),
        out_shape=(pltpu.VMEM((cx, 2, cy, LANES), f32), wide(cz)),
        in_specs=[pl.BlockSpec(memory_space=pltpu.HBM)] * 7,
        out_specs=(near, near),
        scratch_shapes=scratch,
        compiler_params=pltpu.CompilerParams(
            collective_id=0, has_side_effects=True, vmem_limit_bytes=56 * 1024 * 1024),
    )(volume, *[jnp.asarray(w) for w in weights])
    return pl.pallas_call(
        finish,
        out_shape=jax.ShapeDtypeStruct(volume.shape, f32),
        in_specs=[near, near],
        out_specs=pl.BlockSpec(memory_space=pltpu.HBM),
        scratch_shapes=[vmem(cx, cy, cz), pltpu.SemaphoreType.DMA((cx // 8,))],
        compiler_params=pltpu.CompilerParams(vmem_limit_bytes=16 * 1024 * 1024),
    )(rows, v1)


def solution(mesh):
    spec = P("gx", "gy", None)
    body = functools.partial(on_device, mesh.shape["gx"], mesh.shape["gy"])
    return jax.shard_map(body, mesh=mesh, in_specs=(spec,), out_specs=spec, check_vma=False)
```

```python
import functools
import math

import jax
import jax.numpy as jnp
import numpy as np
from jax import lax
from jax.experimental import pallas as pl
from jax.experimental.pallas import tpu as pltpu
from jax.sharding import PartitionSpec as P

ROOT3 = math.sqrt(3.0)
NEAR = math.sqrt(3.0) / 4.0
FAR = (math.sqrt(3.0) - 2.0) / 4.0
LOW = (math.sqrt(3.0) - 1.0) / math.sqrt(2.0)
HIGH = (math.sqrt(3.0) + 1.0) / math.sqrt(2.0)
LANES = 128
PAD = 8


def forward_matrix(size):
    lines = np.eye(size)
    even, odd = lines[:, 0::2], lines[:, 1::2]
    smooth = even + ROOT3 * odd
    detail = odd - NEAR * smooth - FAR * np.roll(smooth, 1, 1)
    smooth = smooth - np.roll(detail, -1, 1)
    return np.concatenate([LOW * smooth, HIGH * detail], 1)


def inverse_matrix(size):
    lines = np.eye(size)
    smooth, detail = lines[:, : size // 2] / LOW, lines[:, size // 2 :] / HIGH
    first = smooth + np.roll(detail, -1, 1)
    odd = detail + NEAR * first + FAR * np.roll(first, 1, 1)
    even = first - ROOT3 * odd
    return np.stack([even, odd], 2).reshape(size, size)


def halves(matrix, size):
    full = np.zeros((size, size))
    full[: matrix.shape[0], : matrix.shape[1]] = matrix
    high = full.astype(jnp.bfloat16)
    low = (full - high.astype(np.float64)).astype(jnp.bfloat16)
    return np.stack([high, low])


def times(values, w_ref):
    high = values.astype(jnp.bfloat16)
    low = (values - high.astype(jnp.float32)).astype(jnp.bfloat16)
    dot = functools.partial(jnp.dot, preferred_element_type=jnp.float32)
    return dot(high, w_ref[0]) + (dot(low, w_ref[0]) + dot(high, w_ref[1]))


def shrink(values, noise):
    return values - jnp.clip(values, -noise, noise)


def sums(even, odd):
    smooth = even + ROOT3 * odd
    return smooth, odd - NEAR * smooth


def undo(detail, first, before):
    odd = detail + NEAR * first + FAR * before
    return first - ROOT3 * odd, odd


def weave(even, odd):
    both = jnp.stack([even, odd], axis=1)
    return both.reshape((2 * even.shape[0],) + even.shape[1:])


def forward_rows(even, odd):
    axis = even.ndim - 2
    smooth, part = sums(even, odd)
    detail = part - FAR * pltpu.roll(smooth, 1, axis)
    return HIGH * detail, LOW * (smooth - pltpu.roll(detail, even.shape[axis] - 1, axis))


def kernel(shape, count_all, nx, ny, vol, g1, g2, g3, g4, g5, g6, o1, v1,
           w1, w2, w3, v2, v3,
           e1, hx1, sx1, hy1, sy1, hc1, sc1, xd1, xs1, s1s, s1d, d1s, d1d,
           e2, ht2, st2, xd2, xs2, ss, sd, ds, dd, ep3, t3d, t3s, r2, r1,
           p1s, p1d, part, total, send, recv, lsem, wsem):
    cx, cy, cz = shape
    hx, hy, qx, qy = cx // 2, cy // 2, cx // 4, cy // 4
    ix, iy = lax.axis_index("gx"), lax.axis_index("gy")

    def device(dx, dy):
        return (lax.rem(ix + dx + nx, nx), lax.rem(iy + dy + ny, ny))

    loads = [
        pltpu.make_async_copy(
            vol.at[:, :, pl.ds(h * LANES, LANES)],
            e1.at[:, h, pl.ds(PAD, cy), :], lsem.at[h])
        for h in range(2)
    ]
    weights = [
        pltpu.make_async_copy(src, dst, wsem.at[i])
        for i, (src, dst) in enumerate(
            zip((g1, g2, g3, g4, g5, g6), (w1, w2, w3, v1, v2, v3)))
    ]
    for c in loads + weights:
        c.start()

    greet = [(dx, dy) for dx in (-1, 0, 1) for dy in (-1, 0, 1) if dx or dy]
    greet += [(dx, 0) for dx in range(2, nx - 1)] + [(0, dy) for dy in range(2, ny - 1)]
    barrier = pltpu.get_barrier_semaphore()
    for d in greet:
        pl.semaphore_signal(barrier, inc=1, device_id=device(*d),
                            device_id_type=pl.DeviceIdType.MESH)

    slot = [0]
    started = []

    def post(src, dst, dx, dy):
        n = slot[0]
        slot[0] += 1
        c = pltpu.make_async_remote_copy(
            src_ref=src, dst_ref=dst, send_sem=send.at[n], recv_sem=recv.at[n],
            device_id=device(dx, dy), device_id_type=pl.DeviceIdType.MESH)
        c.start()
        started.append(c)
        return c

    for c in loads:
        c.wait()

    top = PAD + cy
    sx1[1] = sums(e1[0, :, PAD:top], e1[1, :, PAD:top])[1]
    sy1[1] = sums(e1[:, :, PAD : PAD + 1], e1[:, :, PAD + 1 : PAD + 2])[1]
    sx1[0] = sums(e1[cx - 2, :, PAD:top], e1[cx - 1, :, PAD:top])[0]
    sy1[0] = sums(e1[:, :, top - 2 : top - 1], e1[:, :, top - 1 : top])[0]
    for x in range(2):
        sc1[x, 1] = sums(sx1[x, :, 0:1], sx1[x, :, 1:2])[1]
        sc1[x, 0] = sums(sx1[x, :, cy - 2 : cy - 1], sx1[x, :, cy - 1 : cy])[0]
    pl.semaphore_wait(barrier, len(greet))
    step = (1, -1)
    post_x = lambda x: post(sx1.at[x], hx1.at[x, :, pl.ds(PAD, cy), :], step[x], 0)
    post_y = lambda y: post(sy1.at[y], hy1.at[y], 0, step[y])
    post_c = lambda x, y: post(sc1.at[x, y], hc1.at[x, y], step[x], step[y])
    now1 = [post_c(1, 1), post_x(1), post_y(1)]
    later1 = [post_c(0, 1), post_c(1, 0), post_c(0, 0), post_x(0), post_y(0)]

    def place(ref, rows, side):
        if side == 0:
            ref[..., PAD - 2 : PAD - 1, :] = rows
            ref[..., PAD - 1 : PAD, :] = jnp.zeros_like(rows)
        else:
            ref[..., top : top + 1, :] = -ROOT3 * rows
            ref[..., top + 1 : top + 2, :] = rows

    def pair1(n, rows=slice(None)):
        return sums(e1[2 * n, :, rows], e1[2 * n + 1, :, rows])

    def lift1(rows):
        def step(n, carry):
            _, part_n = pair1(n, rows)
            before, _ = pair1(n - 1, rows)
            detail = part_n - FAR * before
            xd1[n, :, rows] = HIGH * detail
            xs1[n, :, rows] = LOW * (before - detail)
            return carry

        lax.fori_loop(1, hx, step, 0)

    def coarse1(n, first, count):
        for h in range(2):
            load = lambda start: xs1[n, h, pl.ds(start + 2 * first, count, stride=2), :]
            s0, _ = sums(load(PAD), load(PAD + 1))
            _, tp = sums(load(PAD + 2), load(PAD + 3))
            s1s[n, h, PAD + first : PAD + first + count] = LOW * (s0 - (tp - FAR * s0))

    def coarse1_inner(n, carry):
        coarse1(n, 0, hy)
        return carry

    def coarse1_top(n, carry):
        coarse1(n, hy - 1, 1)
        return carry

    lift1(slice(PAD, top))
    lax.fori_loop(1, hx, coarse1_inner, 0)
    for c in weights:
        c.wait()
    for c in now1:
        c.wait_recv()
    place(e1, hy1[1], 1)
    place(hx1.at[1], hc1[1, 1], 1)
    lift1(slice(top, top + 2))
    edge, _ = pair1(hx - 1)
    edge_d = hx1[1] - FAR * edge
    xd1[hx] = HIGH * edge_d
    xs1[hx] = LOW * (edge - edge_d)
    lax.fori_loop(1, hx, coarse1_top, 0)
    coarse1(hx, 0, hy)

    def lines(ref, xs, ys):
        n = (xs.stop - xs.start) * (ys.stop - ys.start)
        return jnp.concatenate([ref[xs, h, ys].reshape(n, LANES) for h in range(2)], axis=1)

    chunk = hx // 2
    for i in range(2):
        rows = lines(s1s, slice(1 + i * chunk, 1 + (i + 1) * chunk), slice(PAD, PAD + hy))
        e2[4 + i * chunk : 4 + (i + 1) * chunk, PAD : PAD + hy] = times(
            rows, w1.at[:, :, 0:LANES]).reshape(chunk, hy, LANES)

    st2[...] = sums(e2[4, PAD : PAD + hy], e2[5, PAD : PAD + hy])[1]
    y_own, y_low, y_high = pl.ds(PAD, hy), pl.ds(0, PAD), pl.ds(PAD + hy, PAD)
    y_first, y_last = pl.ds(PAD, PAD), pl.ds(hy, PAD)
    own2, from2, to2 = pl.ds(4, hx), pl.ds(hx, 4), pl.ds(0, 4)
    now2 = [
        post(st2, ht2.at[y_own, :], -1, 0),
        post(e2.at[own2, y_first, :], e2.at[own2, y_high, :], 0, -1),
        post(st2.at[pl.ds(0, PAD), :], ht2.at[y_high, :], -1, -1),
    ]
    later2 = [
        post(e2.at[own2, y_last, :], e2.at[own2, y_low, :], 0, 1),
        post(e2.at[from2, y_own, :], e2.at[to2, y_own, :], 1, 0),
        post(e2.at[from2, y_last, :], e2.at[to2, y_low, :], 1, 1),
        post(e2.at[from2, y_first, :], e2.at[to2, y_high, :], 1, -1),
        post(st2.at[pl.ds(hy - PAD, PAD), :], ht2.at[y_low, :], -1, 1),
    ]

    for c in later1:
        c.wait_recv()
    place(e1, hy1[0], 0)
    place(hx1.at[1], hc1[1, 0], 0)
    place(hx1.at[0], hc1[0, 0], 0)
    place(hx1.at[0], hc1[0, 1], 1)
    first_s, first_t = pair1(0)
    first_d = first_t - FAR * hx1[0]
    xd1[0] = HIGH * first_d
    xs1[0] = LOW * (hx1[0] - first_d)
    low = slice(PAD - 2, PAD)

    lift1(low)
    edge, _ = sums(e1[cx - 2, :, low], e1[cx - 1, :, low])
    edge_d = hx1[1, :, low] - FAR * edge
    xd1[hx, :, low] = HIGH * edge_d
    xs1[hx, :, low] = LOW * (edge - edge_d)

    def cols1(src, det, smo):
        def step(n, carry):
            for h in range(2):
                load = lambda start: src[n, h, pl.ds(start, hy + 1, stride=2), :]
                s0, t0 = sums(load(PAD), load(PAD + 1))
                sm, _ = sums(load(PAD - 2), load(PAD - 1))
                d = t0 - FAR * sm
                det[n, h, 0 : hy + 1] = HIGH * d
                smo[n, h, PAD - 1 : PAD + hy] = LOW * (sm - d)
            return carry

        lax.fori_loop(0, hx + 1, step, 0)

    rows1 = hy + PAD
    parts1 = ((0, chunk), (chunk, hx + 1))

    def depth1(ref):
        magnitude = jnp.zeros((PAD, LANES), jnp.float32)
        for lo, hi in parts1:
            rows = lines(ref, slice(lo, hi), slice(0, rows1))
            if ref is s1s:
                ref[lo:hi, 1] = times(rows, w1.at[:, :, LANES : 2 * LANES]).reshape(
                    hi - lo, rows1, LANES)
                continue
            got = times(rows, w1)
            for h in range(2):
                ref[lo:hi, h] = got[:, h * LANES : (h + 1) * LANES].reshape(hi - lo, rows1, LANES)
            if ref is d1d:
                mine = got[:, LANES:].reshape(hi - lo, rows1, LANES)[:chunk, :hy]
                magnitude = magnitude + jnp.sum(
                    jnp.abs(mine).reshape(chunk * hy // PAD, PAD, LANES), axis=0)
        return magnitude

    cols1(xd1, d1d, d1s)
    part[0] = depth1(d1d)
    sums_x = [post(part.at[0], part.at[k], k, 0) for k in range(1, nx)]

    for c in now2:
        c.wait_recv()
    x2, yrows, pairs = qx + 2, qy + 2 * PAD, hy // 2 + PAD

    def lift2(rows):
        def step(n, carry):
            before, _ = sums(e2[2 * n, rows], e2[2 * n + 1, rows])
            _, part_n = sums(e2[2 * n + 2, rows], e2[2 * n + 3, rows])
            detail = part_n - FAR * before
            xd2[n, rows] = HIGH * detail
            xs2[n, rows] = LOW * (before - detail)
            return carry
        return step

    def last2(rows):
        before, _ = sums(e2[2 * x2 - 2, rows], e2[2 * x2 - 1, rows])
        detail = ht2[rows] - FAR * before
        xd2[x2 - 1, rows] = HIGH * detail
        xs2[x2 - 1, rows] = LOW * (before - detail)

    above, every = slice(PAD, hy + 2 * PAD), slice(0, hy + 2 * PAD)
    lax.fori_loop(2, x2 - 1, lift2(above), 0)
    last2(above)
    load2 = lambda start: xs2[2:x2, pl.ds(start, qy, stride=2), :]
    s0, _ = sums(load2(PAD), load2(PAD + 1))
    _, tp = sums(load2(PAD + 2), load2(PAD + 3))
    smooth2 = LOW * (s0 - (tp - FAR * s0))
    coarse2 = times(smooth2.reshape(qx * qy, LANES), w2)
    coarse2 = coarse2.reshape(qx // 2, 2, qy, LANES)
    lane = lax.broadcasted_iota(jnp.int32, (qx // 2, qy, LANES), 2)
    half = LANES // 2
    packed = jnp.where(lane < half, coarse2[:, 0], pltpu.roll(coarse2[:, 1], half, 2))
    ep3[2 : 2 + qx // 2, PAD : PAD + qy] = packed

    n_own = qx // 2
    own3 = pl.ds(2, n_own)
    z_own, z_low, z_high = pl.ds(PAD, qy), pl.ds(0, PAD), pl.ds(PAD + qy, PAD)
    z_first, z_last = pl.ds(PAD, PAD), pl.ds(qy, PAD)
    round3 = []
    for dx, xs, xd in ((1, pl.ds(n_own, 2), pl.ds(0, 2)),
                       (-1, pl.ds(2, 1), pl.ds(2 + n_own, 1)), (0, own3, own3)):
        for dy, ys, yd in ((0, z_own, z_own), (1, z_last, z_low), (-1, z_first, z_high)):
            if dx or dy:
                round3.append(post(ep3.at[xs, ys, :], ep3.at[xd, yd, :], dx, dy))

    cols1(xs1, s1d, s1s)
    depth1(d1s)

    for c in sums_x:
        c.wait_recv()
    acc = part[0]
    for k in range(1, nx):
        acc = acc + part[k]
    total[0] = acc
    sums_y = [post(total.at[0], total.at[k], 0, k) for k in range(1, ny)]

    depth1(s1d)
    depth1(s1s)

    for c in later2:
        c.wait_recv()
    lax.fori_loop(0, x2 - 1, lift2(every), 0)
    last2(every)

    def rows2(src, at):
        return forward_rows(src[at, pl.ds(0, pairs, stride=2), :],
                            src[at, pl.ds(1, pairs, stride=2), :])

    for src, det, smo in ((xd2, dd, ds), (xs2, sd, ss)):
        for band, dst in zip(rows2(src, slice(0, x2)), (det, smo)):
            dst[:, PAD // 2 : PAD // 2 + pairs] = times(
                band.reshape(x2 * pairs, LANES), w2).reshape(x2, pairs, LANES)

    for c in round3:
        c.wait_recv()
    low_s, low_t = [], []
    for n in range(n_own + 3):
        s, t = sums(ep3[n], pltpu.roll(ep3[n], half, 1))
        low_s.append(s)
        low_t.append(t)
    n3 = n_own + 2
    for n in range(n3):
        detail = low_t[n + 1] - FAR * low_s[n]
        t3d[n] = HIGH * detail
        t3s[n] = LOW * (low_s[n] - detail)
    h3 = qy // 2 + PAD
    bands = []
    for src in (t3d, t3s):
        bands += forward_rows(src[:, pl.ds(0, h3, stride=2), :], src[:, pl.ds(1, h3, stride=2), :])
    for i, band in enumerate(bands):
        bands[i] = times(band.reshape(n3 * h3, LANES), w3).reshape(n3, h3, LANES)

    for c in sums_y:
        c.wait_recv()
    acc = total[0]
    for k in range(1, ny):
        acc = acc + total[k]
    noise = jnp.sum(acc, axis=(0, 1), keepdims=True) * (math.sqrt(math.pi / 2.0) / count_all)

    lane3 = lax.broadcasted_iota(jnp.int32, (n3, h3, LANES), 2)
    noise3 = noise.reshape(1, 1, 1)
    b_dd, b_ds, b_sd = (shrink(b, noise3) for b in bands[:3])
    b_ss = jnp.where(lane3 < cz // 8, bands[3], shrink(bands[3], noise3))

    def inverse_x(det, smo):
        det, smo = det * (1.0 / HIGH), smo * (1.0 / LOW)
        one = smo + det
        even, odd = undo(det[:-1], one[1:], one[:-1])
        return weave(even, odd)

    y_d = inverse_x(b_dd, b_sd) * (1.0 / HIGH)
    y_s = inverse_x(b_ds, b_ss) * (1.0 / LOW)
    one = y_s + pltpu.roll(y_d, h3 - 1, 1)
    even, odd = undo(y_d, one, pltpu.roll(one, 1, 1))
    r2[:, pl.ds(0, h3, stride=2), :] = even
    r2[:, pl.ds(1, h3, stride=2), :] = odd
    back = times(r2[...].reshape(x2 * yrows, LANES), v3).reshape(x2, yrows, LANES)

    lane2 = lax.broadcasted_iota(jnp.int32, (x2, yrows, LANES), 2)
    ss[...] = jnp.where(lane2 < cz // 4, back, shrink(ss[...], noise3))

    def inv2(n, carry):
        def one_x(n):
            d_d = shrink(dd[n], noise) * (1.0 / HIGH)
            d_s = shrink(ds[n], noise) * (1.0 / HIGH)
            s_d = shrink(sd[n], noise) * (1.0 / LOW)
            s_s = ss[n] * (1.0 / LOW)
            return d_d, d_s, s_d + d_d, s_s + d_s

        d_d, d_s, b_d, b_s = one_x(n)
        _, _, f_d, f_s = one_x(n + 1)
        pair_d = undo(d_d, f_d, b_d)
        pair_s = undo(d_s, f_s, b_s)
        for i in range(2):
            y_d, y_s = pair_d[i] * (1.0 / HIGH), pair_s[i] * (1.0 / LOW)
            one = y_s + pltpu.roll(y_d, yrows - 1, 0)
            even, odd = undo(y_d, one, pltpu.roll(one, 1, 0))
            r1[2 * n + i, pl.ds(0, yrows, stride=2), :] = even
            r1[2 * n + i, pl.ds(1, yrows, stride=2), :] = odd
        return carry

    lax.fori_loop(0, qx + 1, inv2, 0)
    x1, y1 = hx + 2, hy + PAD
    back = times(r1[:, PAD : PAD + y1].reshape(x1 * y1, LANES), v2).reshape(x1, y1, LANES)
    s1s[:, 0] = back[1:]

    def inv1(n, carry):
        for h in range(2):
            for det, smo, dst in ((d1d, s1d, p1d), (d1s, s1s, p1s)):
                plain = smo is s1s and h == 0

                def one_x(n):
                    d = shrink(det[n, h], noise) * (1.0 / HIGH)
                    s = smo[n, h] if plain else shrink(smo[n, h], noise)
                    return d, s * (1.0 / LOW) + d

                d, before = one_x(n)
                _, one = one_x(n + 1)
                even, odd = undo(d, one, before)
                dst[2 * n, h] = even
                dst[2 * n + 1, h] = odd
        return carry

    lax.fori_loop(0, hx, inv1, 0)

    def inv1_y(n, carry):
        for h in range(2):
            y_d = p1d[n, h, 0:hy] * (1.0 / HIGH)
            y_n = p1d[n, h, 1 : hy + 1] * (1.0 / HIGH)
            s = p1s[n, h, PAD : PAD + hy] * (1.0 / LOW)
            s_b = p1s[n, h, PAD - 1 : PAD - 1 + hy] * (1.0 / LOW)
            even, odd = undo(y_d, s + y_n, s_b + y_d)
            o1[n, h, pl.ds(0, hy, stride=2), :] = even
            o1[n, h, pl.ds(1, hy, stride=2), :] = odd
        return carry

    lax.fori_loop(0, cx, inv1_y, 0)
    for c in started:
        c.wait_send()


def finish(rows_in, v1, out, ob, osem):
    cx, cy, cz = out.shape
    layers = 8
    outs = []
    for i in range(cx // layers):
        xs = slice(i * layers, (i + 1) * layers)
        rows = jnp.concatenate(
            [rows_in[xs, h].reshape(layers * cy, LANES) for h in range(2)], axis=1)
        ob[xs] = times(rows, v1).reshape(layers, cy, cz)
        c = pltpu.make_async_copy(ob.at[xs], out.at[xs], osem.at[i])
        c.start()
        outs.append(c)
    for c in outs:
        c.wait()


def on_device(nx, ny, volume):
    cx, cy, cz = volume.shape
    hx, hy, qx, qy = cx // 2, cy // 2, cx // 4, cy // 4
    n3, h3 = qx // 2 + 2, qy // 2 + PAD
    f32 = jnp.float32
    count = cx * nx * cy * ny * cz // 8
    weights = [
        halves(forward_matrix(cz), cz), halves(forward_matrix(cz // 2), LANES),
        halves(forward_matrix(cz // 4), LANES), halves(inverse_matrix(cz), cz),
        halves(inverse_matrix(cz // 2), LANES), halves(inverse_matrix(cz // 4), LANES),
    ]
    messages = 24 + nx - 1 + ny - 1
    vmem = lambda *s: pltpu.VMEM(s, f32)
    ey, ey2, ey3 = cy + 2 * PAD, hy + 2 * PAD, qy + 2 * PAD
    wide = lambda n: pltpu.VMEM((2, n, n), jnp.bfloat16)
    scratch = [
        wide(cz), wide(LANES), wide(LANES), wide(LANES), wide(LANES),
        vmem(cx, 2, ey, LANES), vmem(2, 2, ey, LANES), vmem(2, 2, cy, LANES),
        vmem(2, cx, 2, 1, LANES), vmem(2, cx, 2, 1, LANES),
        vmem(2, 2, 2, 1, LANES), vmem(2, 2, 2, 1, LANES),
        vmem(hx + 1, 2, ey, LANES), vmem(hx + 1, 2, ey, LANES),
        *[vmem(hx + 1, 2, hy + PAD, LANES) for _ in range(4)],
        vmem(hx + 4, ey2, LANES), vmem(ey2, LANES), vmem(hy, LANES),
        vmem(qx + 2, ey2, LANES), vmem(qx + 2, ey2, LANES),
        *[vmem(qx + 2, ey3, LANES) for _ in range(4)],
        vmem(qx // 2 + 3, ey3, LANES),
        vmem(n3, ey3, LANES), vmem(n3, ey3, LANES),
        vmem(qx + 2, ey3, LANES),
        vmem(hx + 2, 2 * ey3, LANES),
        vmem(cx, 2, hy + PAD, LANES), vmem(cx, 2, hy + PAD, LANES),
        vmem(nx, PAD, LANES), vmem(ny, PAD, LANES),
        pltpu.SemaphoreType.DMA((messages,)), pltpu.SemaphoreType.DMA((messages,)),
        pltpu.SemaphoreType.DMA((2,)), pltpu.SemaphoreType.DMA((6,)),
    ]
    near = pl.BlockSpec(memory_space=pltpu.VMEM)
    rows, v1 = pl.pallas_call(
        functools.partial(kernel, (cx, cy, cz), count, nx, ny),
        out_shape=(pltpu.VMEM((cx, 2, cy, LANES), f32), wide(cz)),
        in_specs=[pl.BlockSpec(memory_space=pltpu.HBM)] * 7,
        out_specs=(near, near),
        scratch_shapes=scratch,
        compiler_params=pltpu.CompilerParams(
            collective_id=0, has_side_effects=True, vmem_limit_bytes=56 * 1024 * 1024),
    )(volume, *[jnp.asarray(w) for w in weights])
    return pl.pallas_call(
        finish,
        out_shape=jax.ShapeDtypeStruct(volume.shape, f32),
        in_specs=[near, near],
        out_specs=pl.BlockSpec(memory_space=pltpu.HBM),
        scratch_shapes=[vmem(cx, cy, cz), pltpu.SemaphoreType.DMA((cx // 8,))],
        compiler_params=pltpu.CompilerParams(vmem_limit_bytes=16 * 1024 * 1024),
    )(rows, v1)


def solution(mesh):
    spec = P("gx", "gy", None)
    body = functools.partial(on_device, mesh.shape["gx"], mesh.shape["gy"])
    return jax.shard_map(body, mesh=mesh, in_specs=(spec,), out_specs=spec, check_vma=False)
```
